32 devices in a mesh: section: 4 (over y, x), fsdp: 8 (over z, core).
Axes of the slice: x: 2, y: 2, z: 4, core: 2. Of those that a mesh axis runs over, the one named last changes fastest.
Arguments:
- patches: bfloat16 [8, 1024, 768], P(None, 'fsdp'), may hold values from -6 to 6
- cotangent: bfloat16 [8, 1024, 768], P(None, 'fsdp'), may hold values from -6 to 6
- embed_blocks: int32 [8], replicated, may hold values from 4 to 6
- ratio_index: int32 [8], replicated, may hold values from 0 to 2
- depth: int32 [8], replicated, may hold values from 2 to 4
- w_up: bfloat16 [4, 768, 3072], P('section', 'fsdp'), may hold values from -0.21875 to 0.21875
- w_down: bfloat16 [4, 3072, 768], P('section', 'fsdp'), may hold values from -0.109375 to 0.109375
- ln_gain: bfloat16 [4, 768], P('section', 'fsdp'), may hold values from 0.099609375 to 1.8984375
Outputs:
- grad_up: float32 [4, 768, 3072], P('section', 'fsdp')
- grad_down: float32 [4, 3072, 768], P('section', 'fsdp')
- grad_gain: float32 [4, 768], P('section', 'fsdp')
The draws below stay inside these ranges and needn't reach their ends.
All inputs are finite; a program needn't handle non-finite values.
Results may differ from the reference program's by a relative error of at most 0.028.
Values may be sent and summed in bfloat16 or wider, within the bound.
A program may use at most 192 MiB of HBM per device.

```python
import jax
import jax.numpy as jnp
from jax import lax

D = 768
FF = 3072
BLOCK = 128
MICRO = 8
LAYERS = 4
TOKENS = 1024
N_SECTION = 4


def plant(values, stream_key, low, top_value):
    longest = values.shape.index(max(values.shape))
    spots = []
    for shift in (0, 1):
        where = [jax.random.randint(jax.random.fold_in(stream_key, axis), (), 0, length) for axis, length in enumerate(values.shape)]
        where[longest] = (where[longest] + shift) % values.shape[longest]
        spots.append(tuple(where))
    return values.at[spots[0]].set(low).at[spots[1]].set(top_value)


def strengthened(entries, own_key, source, target, blocks, factor):
    def block_of(position):
        return (jnp.arange(entries.shape[position]) // (entries.shape[position] // blocks)).reshape((-1,) + (1,) * (entries.ndim - 1 - position))

    first = jax.random.permutation(own_key, blocks)[block_of(target)]
    far = (block_of(target) + blocks // 2) % blocks
    return jnp.where((block_of(source) == first) | (block_of(source) == far), factor * entries, entries)


def level_of(stream_key, dims, split, least, high):
    gain = 1.0
    for axis_at, parts in split:
        steps = jax.random.uniform(jax.random.fold_in(jax.random.fold_in(stream_key, 6), axis_at), (parts,), jnp.float32, least / len(split), high / len(split))
        gain = gain * jnp.repeat(jnp.exp(steps), dims[axis_at] // parts).reshape((-1,) + (1,) * (len(dims) - 1 - axis_at))
    return gain


def scatter_about(rng, extent, spread, limit, cuts=(), dtype=jnp.bfloat16):
    values = jax.random.normal(rng, extent, jnp.float32) * spread
    if len(cuts) > 0:
        values = level_of(rng, extent, cuts, -0.22, 0.18) * values
    return jnp.clip(values, min=-limit, max=limit).astype(dtype)


def bell_draw_with(rng, shape, scale, bound, shards, heavy, dtype=jnp.bfloat16):
    entries = scale * jax.random.normal(rng, shape, jnp.float32)
    if shards:
        entries = entries * level_of(rng, shape, shards, -0.22, 0.18)
    return jnp.clip(strengthened(entries, jax.random.fold_in(rng, 3), *heavy), -bound, bound).astype(dtype)


def setup_inputs(seed: int = 0) -> dict:
    seeds = jax.random.split(jax.random.key(seed), 9)
    return {
        "patches": scatter_about(seeds[0], (MICRO, TOKENS, D), 1.0, 6.0, ((1, 8),)),
        "cotangent": bell_draw_with(seeds[1], (MICRO, TOKENS, D), 1.0, 6.0, ((1, 8),), (1, 2, 8, 2.0)),
        "embed_blocks": plant(jax.random.randint(seeds[2], (MICRO,), D // BLOCK - 2, D // BLOCK + 1), jax.random.fold_in(seeds[2], 1), D // BLOCK - 2, (D // BLOCK + 1) - 1).astype(jnp.int32),
        "ratio_index": plant(jax.random.randint(seeds[3], (MICRO,), 0, 3), jax.random.fold_in(seeds[3], 1), 0, 2).astype(jnp.int32),
        "depth": plant(jax.random.randint(seeds[4], (MICRO,), N_SECTION - 2, N_SECTION + 1), jax.random.fold_in(seeds[4], 1), N_SECTION - 2, N_SECTION).astype(jnp.int32),
        "w_up": scatter_about(seeds[5], (LAYERS, D, FF), D ** -0.5, 0.21875, ((0, 4), (1, 8))),
        "w_down": scatter_about(seeds[6], (LAYERS, FF, D), FF ** -0.5, 0.109375, ((0, 4), (1, 8))),
        "ln_gain": jnp.clip(1.0 + 0.18 * jax.random.normal(seeds[7], (LAYERS, D), jnp.float32), 0.099609375, 1.8984375).astype(jnp.bfloat16),
    }


EPSILON = 1e-05

def micro_masks(blocks, ratio, feature_count, hidden_count):
    width_int = (blocks * BLOCK).astype(jnp.int32)
    hidden_int = (width_int * (6 + ratio) // 2).astype(jnp.int32)
    embed_mask = (lax.iota(jnp.int32, feature_count) < width_int).astype(jnp.float32)
    hidden_mask = (lax.iota(jnp.int32, hidden_count) < hidden_int).astype(jnp.float32)
    return (embed_mask, hidden_mask, width_int.astype(jnp.float32))

def layer_norm(inputs, embed_mask, width_float):
    values = inputs.astype(jnp.float32) * embed_mask
    center_value = lax.optimization_barrier(jnp.sum(values, axis=-1, keepdims=True)) / width_float
    centered = (values - center_value) * embed_mask
    variance = lax.optimization_barrier(jnp.sum(centered * centered, axis=-1, keepdims=True)) / width_float
    inv_std = lax.rsqrt(variance + EPSILON)
    return (centered * inv_std, inv_std)

def layer_forward(inputs, gain_vector, weight_up, weight_down, embed_mask, hidden_mask, active, width_float):
    standard, inv_std = layer_norm(inputs, embed_mask, width_float)
    normed = (standard * gain_vector.astype(jnp.float32)).astype(jnp.bfloat16)
    hidden = jnp.dot(normed, weight_up, preferred_element_type=jnp.float32)
    activated = (jax.nn.gelu(hidden) * hidden_mask).astype(jnp.bfloat16)
    branch = jnp.dot(activated, weight_down, preferred_element_type=jnp.float32)
    output = (inputs.astype(jnp.float32) + active * embed_mask * branch).astype(jnp.bfloat16)
    return (output, hidden)

def layer_backward(inputs, hidden, grad_out, gain_vector, weight_up, weight_down, embed_mask, hidden_mask, active, width_float):
    standard, inv_std = layer_norm(inputs, embed_mask, width_float)
    gain_float = gain_vector.astype(jnp.float32)
    normed = (standard * gain_float).astype(jnp.bfloat16)
    activated = (jax.nn.gelu(hidden) * hidden_mask).astype(jnp.bfloat16)
    grad_branch = (active * embed_mask * grad_out.astype(jnp.float32)).astype(jnp.bfloat16)
    grad_act = lax.dot_general(grad_branch, weight_down, (((1,), (1,)), ((), ())), preferred_element_type=jnp.float32)
    unused, pullback = jax.vjp(jax.nn.gelu, hidden)
    grad_hidden = pullback(grad_act * hidden_mask)[0].astype(jnp.bfloat16)
    grad_normed = lax.dot_general(grad_hidden, weight_up, (((1,), (1,)), ((), ())), preferred_element_type=jnp.float32)
    grad_standard = grad_normed * gain_float * embed_mask
    grad_gain = lax.optimization_barrier(jnp.sum(grad_normed * standard, axis=0))
    first_mean = lax.optimization_barrier(jnp.sum(grad_standard, axis=-1, keepdims=True)) / width_float
    second_mean = lax.optimization_barrier(jnp.sum(grad_standard * standard, axis=-1, keepdims=True)) / width_float
    grad_norm_in = inv_std * (grad_standard - first_mean * embed_mask - standard * second_mean)
    grad_in = (grad_out.astype(jnp.float32) + grad_norm_in).astype(jnp.bfloat16)
    return (grad_in, normed, grad_hidden, activated, grad_branch, grad_gain)

def contract_rows(left, right):
    return lax.dot_general(left, right, (((0,), (0,)), ((), ())), preferred_element_type=jnp.float32)

def reference(patches, cotangent, embed_blocks, ratio_index, depth, w_up, w_down, ln_gain):
    feature_count = w_up.shape[1]
    hidden_count = w_up.shape[2]
    grads_up = [jnp.zeros((feature_count, hidden_count), jnp.float32) for layer_number in range(LAYERS)]
    grads_down = [jnp.zeros((hidden_count, feature_count), jnp.float32) for layer_number in range(LAYERS)]
    grads_gain = [jnp.zeros((feature_count,), jnp.float32) for layer_number in range(LAYERS)]
    for micro_number in range(MICRO):
        embed_mask, hidden_mask, width_float = micro_masks(embed_blocks[micro_number], ratio_index[micro_number], feature_count, hidden_count)
        inputs = (patches[micro_number].astype(jnp.float32) * embed_mask).astype(jnp.bfloat16)
        saved = []
        for layer_number in range(LAYERS):
            active = (layer_number < depth[micro_number]).astype(jnp.float32)
            output, hidden = layer_forward(inputs, ln_gain[layer_number], w_up[layer_number], w_down[layer_number], embed_mask, hidden_mask, active, width_float)
            saved.append((inputs, hidden, active))
            inputs = output
        grad_out = (cotangent[micro_number].astype(jnp.float32) * embed_mask).astype(jnp.bfloat16)
        for layer_number in reversed(range(LAYERS)):
            layer_in, hidden, active = saved[layer_number]
            grad_in, normed, grad_hidden, activated, grad_branch, grad_gain = layer_backward(layer_in, hidden, grad_out, ln_gain[layer_number], w_up[layer_number], w_down[layer_number], embed_mask, hidden_mask, active, width_float)
            grads_up[layer_number] = grads_up[layer_number] + contract_rows(normed, grad_hidden)
            grads_down[layer_number] = grads_down[layer_number] + contract_rows(activated, grad_branch)
            grads_gain[layer_number] = grads_gain[layer_number] + grad_gain
            grad_out = grad_in
    return (jnp.stack(grads_up), jnp.stack(grads_down), jnp.stack(grads_gain))
```

```python
import functools

import jax
import jax.numpy as jnp
from jax import lax
from jax.experimental import pallas as pl
from jax.experimental.pallas import tpu as pltpu
from jax.sharding import PartitionSpec as P

BLOCK = 128
EPSILON = 1e-05
SCALE = 0.7978845608028654
MESH = pl.DeviceIdType.MESH
VMEM_BYTES = 66 * 1024 * 1000
BF16 = jnp.bfloat16
F32 = jnp.float32


def gelu_and_slope(hidden):
    square = hidden * hidden
    tanh = jnp.tanh(hidden * (SCALE + (SCALE * 0.044715) * square))
    half = 0.5 + 0.5 * tanh
    rise = (hidden * (0.5 * SCALE + (0.5 * SCALE * 0.134145) * square)) * (1.0 - tanh * tanh)
    return (hidden * half, half + rise)


def contract_last(left, right):
    return lax.dot_general(left, right, (((1,), (1,)), ((), ())), preferred_element_type=F32)


def chunks(total, size):
    size = size if total % size == 0 else total
    return [(start, size) for start in range(0, total, size)]


def pipeline_kernel(
    section_count,
    patches,
    cotangent,
    embed,
    live,
    hidden_mask,
    width_inv,
    gain_ref,
    w_up,
    w_down,
    grad_up,
    grad_down,
    grad_gain,
    x_in,
    x_out,
    g_in,
    g_out,
    act,
    slope,
    normed_t,
    branch_t,
    fwd_send,
    fwd_recv,
    bwd_send,
    bwd_recv,
):
    me = lax.axis_index("section")
    is_first = me == 0
    is_last = me == section_count - 1
    micro_count, rows, features = patches.shape
    hidden_count = w_up.shape[1]

    barrier = pltpu.get_barrier_semaphore()

    @pl.when(jnp.logical_not(is_first))
    def _():
        pl.semaphore_signal(barrier, inc=1, device_id={"section": me - 1}, device_id_type=MESH)

    @pl.when(jnp.logical_not(is_last))
    def _():
        pl.semaphore_signal(barrier, inc=1, device_id={"section": me + 1}, device_id_type=MESH)

    ends = is_first.astype(jnp.int32) + is_last.astype(jnp.int32)
    pl.semaphore_wait(barrier, 2 - ends)

    def forward_copy(m):
        return pltpu.make_async_remote_copy(
            src_ref=x_out.at[m],
            dst_ref=x_in.at[m],
            send_sem=fwd_send.at[m],
            recv_sem=fwd_recv.at[m],
            device_id={"section": jnp.minimum(me + 1, section_count - 1)},
            device_id_type=MESH,
        )

    def backward_copy(m):
        return pltpu.make_async_remote_copy(
            src_ref=g_out.at[m],
            dst_ref=g_in.at[m],
            send_sem=bwd_send.at[m],
            recv_sem=bwd_recv.at[m],
            device_id={"section": jnp.maximum(me - 1, 0)},
            device_id_type=MESH,
        )

    def layer_norm(m):
        mask = embed[m]
        scale = width_inv[m][:, :1]
        values = x_in[m].astype(F32) * mask
        center = jnp.sum(values, axis=-1, keepdims=True) * scale
        centered = (values - center) * mask
        variance = jnp.sum(centered * centered, axis=-1, keepdims=True) * scale
        inv_std = lax.rsqrt(variance + EPSILON)
        return centered * inv_std, inv_std

    gain = gain_ref[...]

    def forward(m, carry):
        at = pl.ds(pl.multiple_of(m * rows, rows), rows)

        @pl.when(is_first)
        def _():
            x_in[m] = (patches[m].astype(F32) * embed[m]).astype(BF16)

        @pl.when(jnp.logical_not(is_first))
        def _():
            forward_copy(m).wait_recv()

        standard, _ = layer_norm(m)
        scaled = standard * gain
        normed = scaled.astype(BF16)
        normed_t[:, at] = jnp.transpose(scaled).astype(BF16)
        for start, size in chunks(hidden_count, 512):
            part = pl.ds(start, size)
            hidden = jnp.dot(normed, w_up[:, part], preferred_element_type=F32)
            value, rise = gelu_and_slope(hidden)
            mask = hidden_mask[m, :, part]
            act[at, part] = (value * mask).astype(BF16)
            slope[at, part] = (rise * mask).astype(BF16)

        @pl.when(jnp.logical_not(is_last))
        def _():
            for start, size in chunks(features, 256):
                part = pl.ds(start, size)
                branch = jnp.dot(act[at, :], w_down[:, part], preferred_element_type=F32)
                out = x_in[m, :, part].astype(F32) + live[m, :, part] * branch
                x_out[m, :, part] = out.astype(BF16)
            forward_copy(m).start()

        return carry

    lax.fori_loop(0, micro_count, forward, 0)
    grad_gain[...] = jnp.zeros_like(grad_gain)

    def backward(m, carry):
        at = pl.ds(pl.multiple_of(m * rows, rows), rows)

        @pl.when(is_last)
        def _():
            g_in[m] = (cotangent[m].astype(F32) * embed[m]).astype(BF16)

        @pl.when(jnp.logical_not(is_last))
        def _():
            backward_copy(m).wait_recv()

        grad_float = g_in[m].astype(F32)
        branch_float = grad_float * live[m]
        branch = branch_float.astype(BF16)
        branch_t[:, at] = jnp.transpose(branch_float).astype(BF16)
        for start, size in chunks(hidden_count, 512):
            part = pl.ds(start, size)
            grad_act = contract_last(branch, w_down[part, :])
            slope[at, part] = (grad_act * slope[at, part].astype(F32)).astype(BF16)
        grad_hidden = slope[at, :]
        grad_normed = jnp.concatenate(
            [
                contract_last(grad_hidden, w_up[pl.ds(start, size), :])
                for start, size in chunks(features, 256)
            ],
            axis=1,
        )
        standard, inv_std = layer_norm(m)
        mask = embed[m]
        scale = width_inv[m][:, :1]
        grad_gain[...] += jnp.sum(grad_normed * standard, axis=0, keepdims=True)

        @pl.when(jnp.logical_not(is_first))
        def _():
            grad_standard = grad_normed * gain * mask
            first = jnp.sum(grad_standard, axis=-1, keepdims=True) * scale
            second = jnp.sum(grad_standard * standard, axis=-1, keepdims=True) * scale
            grad_x = inv_std * (grad_standard - first * mask - standard * second)
            g_out[m] = (grad_float + grad_x).astype(BF16)
            backward_copy(m).start()

        return carry

    lax.fori_loop(0, micro_count, backward, 0)

    width = 256 if hidden_count % 256 == 0 else hidden_count

    def weight_grads(step, carry):
        part = pl.ds(pl.multiple_of(step * width, width), width)
        up = jnp.dot(normed_t[...], slope[:, part], preferred_element_type=F32)
        grad_up[:, part] = up.astype(BF16)
        down = jnp.dot(branch_t[...], act[:, part], preferred_element_type=F32)
        grad_down[part, :] = jnp.transpose(down).astype(BF16)
        return carry

    lax.fori_loop(0, hidden_count // width, weight_grads, 0)

    def drain(m, carry):
        @pl.when(jnp.logical_not(is_last))
        def _():
            forward_copy(m).wait_send()

        @pl.when(jnp.logical_not(is_first))
        def _():
            backward_copy(m).wait_send()

        return carry

    lax.fori_loop(0, micro_count, drain, 0)


def run_pipeline(patches, cotangent, embed, live, hidden_mask, width_inv, gain, w_up, w_down):
    section_count = lax.axis_size("section")
    micro_count, rows, features = patches.shape
    hidden_count = w_up.shape[1]
    vmem = pl.BlockSpec(memory_space=pltpu.VMEM)
    token = (micro_count, rows, features)
    tokens = micro_count * rows
    return pl.pallas_call(
        functools.partial(pipeline_kernel, section_count),
        out_shape=(
            jax.ShapeDtypeStruct((features, hidden_count), BF16),
            jax.ShapeDtypeStruct((hidden_count, features), BF16),
            jax.ShapeDtypeStruct((1, features), F32),
        ),
        in_specs=[vmem] * 9,
        out_specs=(vmem, vmem, vmem),
        scratch_shapes=[
            pltpu.VMEM(token, BF16),
            pltpu.VMEM(token, BF16),
            pltpu.VMEM(token, BF16),
            pltpu.VMEM(token, BF16),
            pltpu.VMEM((tokens, hidden_count), BF16),
            pltpu.VMEM((tokens, hidden_count), BF16),
            pltpu.VMEM((features, tokens), BF16),
            pltpu.VMEM((features, tokens), BF16),
            pltpu.SemaphoreType.DMA((micro_count,)),
            pltpu.SemaphoreType.DMA((micro_count,)),
            pltpu.SemaphoreType.DMA((micro_count,)),
            pltpu.SemaphoreType.DMA((micro_count,)),
        ],
        compiler_params=pltpu.CompilerParams(
            collective_id=0, has_side_effects=True, vmem_limit_bytes=VMEM_BYTES
        ),
    )(patches, cotangent, embed, live, hidden_mask, width_inv, gain, w_up, w_down)


def per_device(patches, cotangent, embed_blocks, ratio_index, depth, w_up, w_down, ln_gain):
    section_index = lax.axis_index("section")
    micro_count, rows, features = patches.shape
    hidden_count = w_up.shape[2]

    width = embed_blocks * BLOCK
    hidden_width = width * (6 + ratio_index) // 2
    embed = (lax.iota(jnp.int32, features)[None, :] < width[:, None]).astype(F32)
    hidden_mask = (lax.iota(jnp.int32, hidden_count)[None, :] < hidden_width[:, None]).astype(F32)
    active = (section_index < depth).astype(F32)
    live = embed * active[:, None]
    width_inv = jnp.broadcast_to((1.0 / width.astype(F32))[:, None, None], (micro_count, 1, BLOCK))

    full_up = lax.all_gather(w_up[0], "fsdp", axis=0, tiled=True)
    full_down = lax.all_gather(w_down[0], "fsdp", axis=0, tiled=True)
    gain = lax.all_gather(ln_gain[0], "fsdp", axis=0, tiled=True).astype(F32)

    part_up, part_down, part_gain = run_pipeline(
        patches,
        cotangent,
        embed[:, None, :],
        live[:, None, :],
        hidden_mask[:, None, :],
        width_inv,
        gain[None],
        full_up,
        full_down,
    )
    own_down = lax.psum_scatter(part_down, "fsdp", scatter_dimension=0, tiled=True)
    own_up = lax.psum_scatter(part_up, "fsdp", scatter_dimension=0, tiled=True)
    own_gain = lax.psum_scatter(part_gain[0], "fsdp", scatter_dimension=0, tiled=True)
    return (own_up.astype(F32)[None], own_down.astype(F32)[None], own_gain[None])


def solution(mesh):
    return jax.shard_map(
        per_device,
        mesh=mesh,
        in_specs=(
            P(None, "fsdp", None),
            P(None, "fsdp", None),
            P(),
            P(),
            P(),
            P("section", "fsdp", None),
            P("section", "fsdp", None),
            P("section", "fsdp"),
        ),
        out_specs=(P("section", "fsdp", None), P("section", "fsdp", None), P("section", "fsdp")),
        check_vma=False,
    )
```

```python
import functools
import math

import jax
import jax.numpy as jnp
from jax import lax
from jax.experimental import pallas as pl
from jax.experimental.pallas import tpu as pltpu
from jax.sharding import PartitionSpec as P

BLOCK = 128
EPSILON = 1e-05
SCALE = 0.7978845608028654
MESH = pl.DeviceIdType.MESH
VMEM_BYTES = 66 * 1024 * 1000
BF16 = jnp.bfloat16
F32 = jnp.float32


def gelu_and_slope(hidden):
    square = hidden * hidden
    tanh = jnp.tanh(hidden * (SCALE + (SCALE * 0.044715) * square))
    half = 0.5 + 0.5 * tanh
    rise = (hidden * (0.5 * SCALE + (0.5 * SCALE * 0.134145) * square)) * (1.0 - tanh * tanh)
    return (hidden * half, half + rise)


def contract_last(left, right):
    return lax.dot_general(left, right, (((1,), (1,)), ((), ())), preferred_element_type=F32)


def chunks(total, size):
    size = size if total % size == 0 else total
    return [(start, size) for start in range(0, total, size)]


def signal(semaphore, device):
    pl.semaphore_signal(semaphore, inc=1, device_id=device, device_id_type=MESH)


def pipeline_kernel(
    section_count,
    shard_count,
    patches,
    cotangent,
    embed,
    live,
    hidden_mask,
    width_inv,
    own_gain,
    own_up,
    own_down,
    grad_up,
    grad_down,
    grad_gain,
    x_in,
    x_out,
    g_in,
    g_out,
    act,
    slope,
    normed_t,
    branch_t,
    fwd_send,
    fwd_recv,
    bwd_send,
    bwd_recv,
    w_up=None,
    w_down=None,
    all_gain=None,
    all_rise=None,
    acc_gain=None,
    pair_up=None,
    pair_down=None,
    line_up=None,
    line_down=None,
    spread_line_send=None,
    spread_line_recv=None,
    spread_pair_send=None,
    spread_pair_recv=None,
    sum_line_send=None,
    sum_line_recv=None,
    sum_pair_send=None,
    sum_pair_recv=None,
):
    inside = w_up is not None
    me = lax.axis_index("section")
    is_first = me == 0
    is_last = me == section_count - 1
    micro_count, rows, features = patches.shape
    shard = lax.axis_index("fsdp")
    chip = shard // 2
    core = shard % 2
    chips = shard_count // 2
    has_below = chip > 0
    has_above = chip < chips - 1
    other = shard + 1 - 2 * core

    barrier = pltpu.get_barrier_semaphore()

    @pl.when(jnp.logical_not(is_first))
    def _():
        signal(barrier, {"section": me - 1})

    @pl.when(jnp.logical_not(is_last))
    def _():
        signal(barrier, {"section": me + 1})

    peers = 2 - is_first.astype(jnp.int32) - is_last.astype(jnp.int32)
    if inside:
        signal(barrier, {"fsdp": other})

        @pl.when(has_below)
        def _():
            signal(barrier, {"fsdp": shard - 2})

        @pl.when(has_above)
        def _():
            signal(barrier, {"fsdp": shard + 2})

        peers = peers + 1 + has_below.astype(jnp.int32) + has_above.astype(jnp.int32)
    pl.semaphore_wait(barrier, peers)

    def slot(full, index):
        if full.ndim == 3:
            return full.at[index]
        size = full.shape[0] // shard_count
        return full.at[pl.ds(pl.multiple_of(index * size, size), size)]

    def line_copy(full, number, source, place, step):
        return pltpu.make_async_remote_copy(
            src_ref=source,
            dst_ref=slot(full, 2 * place + core),
            send_sem=spread_line_send.at[number, (step + 1) // 2, place],
            recv_sem=spread_line_recv.at[number, place],
            device_id={"fsdp": jnp.clip(shard + 2 * step, 0, shard_count - 1)},
            device_id_type=MESH,
        )

    def pair_copy(full, number, source, place):
        return pltpu.make_async_remote_copy(
            src_ref=source,
            dst_ref=slot(full, 2 * place + core),
            send_sem=spread_pair_send.at[number, place],
            recv_sem=spread_pair_recv.at[number, place],
            device_id={"fsdp": other},
            device_id_type=MESH,
        )

    def spread_open(full, number, own):
        @pl.when(has_above)
        def _():
            line_copy(full, number, own, chip, 1).start()

        @pl.when(has_below)
        def _():
            line_copy(full, number, own, chip, -1).start()

        pair_copy(full, number, own, chip).start()
        mine = slot(full, shard)
        mine[...] = own[...]

    def spread_step(full, number, distance):
        below = jnp.maximum(chip - distance, 0)
        above = jnp.minimum(chip + distance, chips - 1)

        @pl.when(chip >= distance)
        def _():
            source = slot(full, 2 * below + core)
            line_copy(full, number, source, below, 1).wait_recv()

            @pl.when(has_above)
            def _():
                line_copy(full, number, source, below, 1).start()

            pair_copy(full, number, source, below).start()

        @pl.when(chip + distance < chips)
        def _():
            source = slot(full, 2 * above + core)
            line_copy(full, number, source, above, -1).wait_recv()

            @pl.when(has_below)
            def _():
                line_copy(full, number, source, above, -1).start()

            pair_copy(full, number, source, above).start()

    def spread_close(full, number):
        for place in range(chips):
            source = slot(full, 2 * place + core)
            pair_copy(full, number, source, place).wait_recv()

    def spread_sent(full, number):
        for place in range(chips):
            source = slot(full, 2 * place + core)
            pair_copy(full, number, source, place).wait_send()

            @pl.when(jnp.logical_and(place <= chip, has_above))
            def _():
                line_copy(full, number, source, place, 1).wait_send()

            @pl.when(jnp.logical_and(place >= chip, has_below))
            def _():
                line_copy(full, number, source, place, -1).wait_send()

    if inside:
        loads = ((w_up, 0, own_up), (w_down, 1, own_down), (all_gain, 2, own_gain))
        for full, number, own in loads:
            spread_open(full, number, own)
        for distance in range(1, chips):
            for full, number, own in loads:
                spread_step(full, number, distance)
        for full, number, own in loads:
            spread_close(full, number)
        gain = jnp.sum(all_gain[...], axis=0)[:1]
    else:
        w_up, w_down, acc_gain = own_up, own_down, grad_gain
        gain = own_gain[:1]
    hidden_count = w_up.shape[1]

    def forward_copy(m):
        return pltpu.make_async_remote_copy(
            src_ref=x_out.at[m],
            dst_ref=x_in.at[m],
            send_sem=fwd_send.at[m],
            recv_sem=fwd_recv.at[m],
            device_id={"section": jnp.minimum(me + 1, section_count - 1)},
            device_id_type=MESH,
        )

    def backward_copy(m):
        return pltpu.make_async_remote_copy(
            src_ref=g_out.at[m],
            dst_ref=g_in.at[m],
            send_sem=bwd_send.at[m],
            recv_sem=bwd_recv.at[m],
            device_id={"section": jnp.maximum(me - 1, 0)},
            device_id_type=MESH,
        )

    def layer_norm(m):
        mask = embed[m]
        scale = width_inv[m][:, :1]
        values = x_in[m].astype(F32) * mask
        center = jnp.sum(values, axis=-1, keepdims=True) * scale
        centered = (values - center) * mask
        variance = jnp.sum(centered * centered, axis=-1, keepdims=True) * scale
        inv_std = lax.rsqrt(variance + EPSILON)
        return centered * inv_std, inv_std

    def forward(m, carry):
        at = pl.ds(pl.multiple_of(m * rows, rows), rows)

        @pl.when(is_first)
        def _():
            x_in[m] = (patches[m].astype(F32) * embed[m]).astype(BF16)

        @pl.when(jnp.logical_not(is_first))
        def _():
            forward_copy(m).wait_recv()

        standard, _ = layer_norm(m)
        scaled = standard * gain
        normed = scaled.astype(BF16)
        normed_t[:, at] = jnp.transpose(scaled).astype(BF16)
        for start, size in chunks(hidden_count, 512):
            part = pl.ds(start, size)
            hidden = jnp.dot(normed, w_up[:, part], preferred_element_type=F32)
            value, rise = gelu_and_slope(hidden)
            mask = hidden_mask[m, :, part]
            act[at, part] = (value * mask).astype(BF16)
            slope[at, part] = (rise * mask).astype(BF16)

        @pl.when(jnp.logical_not(is_last))
        def _():
            for start, size in chunks(features, 256):
                part = pl.ds(start, size)
                branch = jnp.dot(act[at, :], w_down[:, part], preferred_element_type=F32)
                out = x_in[m, :, part].astype(F32) + live[m, :, part] * branch
                x_out[m, :, part] = out.astype(BF16)
            forward_copy(m).start()

        return carry

    lax.fori_loop(0, micro_count, forward, 0)
    acc_gain[...] = jnp.zeros_like(acc_gain)

    def backward(m, carry):
        at = pl.ds(pl.multiple_of(m * rows, rows), rows)

        @pl.when(is_last)
        def _():
            g_in[m] = (cotangent[m].astype(F32) * embed[m]).astype(BF16)

        @pl.when(jnp.logical_not(is_last))
        def _():
            backward_copy(m).wait_recv()

        grad_float = g_in[m].astype(F32)
        branch_float = grad_float * live[m]
        branch = branch_float.astype(BF16)
        branch_t[:, at] = jnp.transpose(branch_float).astype(BF16)
        for start, size in chunks(hidden_count, 512):
            part = pl.ds(start, size)
            grad_act = contract_last(branch, w_down[part, :])
            slope[at, part] = (grad_act * slope[at, part].astype(F32)).astype(BF16)
        grad_hidden = slope[at, :]
        grad_normed = jnp.concatenate(
            [
                contract_last(grad_hidden, w_up[pl.ds(start, size), :])
                for start, size in chunks(features, 256)
            ],
            axis=1,
        )
        standard, inv_std = layer_norm(m)
        mask = embed[m]
        scale = width_inv[m][:, :1]
        acc_gain[...] += jnp.sum((grad_normed * standard).reshape(-1, 8, features), axis=0)

        @pl.when(jnp.logical_not(is_first))
        def _():
            grad_standard = grad_normed * gain * mask
            first = jnp.sum(grad_standard, axis=-1, keepdims=True) * scale
            second = jnp.sum(grad_standard * standard, axis=-1, keepdims=True) * scale
            grad_x = inv_std * (grad_standard - first * mask - standard * second)
            g_out[m] = (grad_float + grad_x).astype(BF16)
            backward_copy(m).start()

        return carry

    lax.fori_loop(0, micro_count, backward, 0)

    width = 256 if hidden_count % 256 == 0 else hidden_count

    def up_grads(first, size, step):
        part = pl.ds(pl.multiple_of(step * width, width), width)
        these = pl.ds(first, size)
        return these, part, jnp.dot(normed_t[these, :], slope[:, part], preferred_element_type=F32)

    def down_grads(part):
        down = jnp.dot(branch_t[...], act[:, part], preferred_element_type=F32)
        return jnp.transpose(down).astype(BF16)

    def weight_grads(step, carry):
        these, part, up = up_grads(0, features, step)
        grad_up[these, part] = up.astype(BF16)
        grad_down[part, :] = down_grads(part)
        return carry

    def sum_pair(full, pair, number, place):
        return pltpu.make_async_remote_copy(
            src_ref=slot(full, 2 * place + 1 - core),
            dst_ref=pair.at[place],
            send_sem=sum_pair_send.at[number, place],
            recv_sem=sum_pair_recv.at[number, place],
            device_id={"fsdp": other},
            device_id_type=MESH,
        )

    def sum_line(full, line, number, place, target, to):
        return pltpu.make_async_remote_copy(
            src_ref=slot(full, 2 * place + core),
            dst_ref=line.at[target],
            send_sem=sum_line_send.at[number, place],
            recv_sem=sum_line_recv.at[number, target],
            device_id={"fsdp": to},
            device_id_type=MESH,
        )

    def reduce_step(index, carry):
        distance = chips - 1 - index // 2
        way = 1 - 2 * (index % 2)
        place = chip + way * distance

        for hops in range(1, chips):

            @pl.when(index == 2 * hops)
            def _():
                spread_step(all_rise, 3, hops)

        @pl.when(jnp.logical_and(place >= 0, place < chips))
        def _():
            up_size = 2 * features // shard_count
            first_row = pl.multiple_of(place * up_size, up_size)

            def up_part(step, carry):
                these, part, up = up_grads(first_row, up_size, step)
                w_up[these, part] = up.astype(BF16)
                return carry

            lax.fori_loop(0, hidden_count // width, up_part, 0)
            sum_pair(w_up, pair_up, 0, place).start()
            down_size = 2 * hidden_count // shard_count

            def down_part(step, carry):
                piece = math.gcd(down_size, width)
                part = pl.ds(pl.multiple_of(place * down_size + step * piece, piece), piece)
                w_down[part, :] = down_grads(part)
                return carry

            lax.fori_loop(0, down_size // math.gcd(down_size, width), down_part, 0)
            sum_pair(w_down, pair_down, 1, place).start()

            is_own = distance == 0
            from_below = jnp.logical_and(place >= chip, has_below)
            from_above = jnp.logical_and(place <= chip, has_above)
            high_slot = jnp.where(is_own, chips, place)
            to = jnp.clip(shard + 2 * way, 0, shard_count - 1)
            target = jnp.where(place == chip - 1, chips, place)
            sets = ((w_up, pair_up, line_up, 0, grad_up), (w_down, pair_down, line_down, 1, grad_down))
            for full, pair, line, number, out in sets:
                mine = slot(full, 2 * place + core)
                sum_pair(full, pair, number, place).wait_recv()

                @pl.when(from_below)
                def _():
                    sum_line(full, line, number, place, place, to).wait_recv()

                @pl.when(from_above)
                def _():
                    sum_line(full, line, number, place, high_slot, to).wait_recv()

                @pl.when(jnp.logical_not(is_own))
                def _():
                    @pl.when(jnp.logical_or(from_below, from_above))
                    def _():
                        total = mine[...].astype(F32) + pair[place].astype(F32)
                        mine[...] = (total + line[place].astype(F32)).astype(BF16)

                    @pl.when(jnp.logical_not(jnp.logical_or(from_below, from_above)))
                    def _():
                        mine[...] = (mine[...].astype(F32) + pair[place].astype(F32)).astype(BF16)

                    sum_line(full, line, number, place, target, to).start()

                @pl.when(is_own)
                def _():
                    out[...] = mine[...].astype(F32) + pair[place].astype(F32)

                    @pl.when(from_below)
                    def _():
                        out[...] += line[place].astype(F32)

                    @pl.when(from_above)
                    def _():
                        out[...] += line[chips].astype(F32)

        return carry

    if inside:
        spread_open(all_rise, 3, acc_gain)
        for full, number, own in loads:
            spread_sent(full, number)
        lax.fori_loop(0, 2 * chips - 1, reduce_step, 0)
        spread_close(all_rise, 3)
        spread_sent(all_rise, 3)
        grad_gain[...] = jnp.sum(all_rise[...], axis=0)
        for place in range(chips):
            for full, pair, line, number in ((w_up, pair_up, line_up, 0), (w_down, pair_down, line_down, 1)):
                sum_pair(full, pair, number, place).wait_send()

                @pl.when(chip != place)
                def _():
                    sum_line(full, line, number, place, place, other).wait_send()
    else:
        lax.fori_loop(0, hidden_count // width, weight_grads, 0)

    def drain(m, carry):
        @pl.when(jnp.logical_not(is_last))
        def _():
            forward_copy(m).wait_send()

        @pl.when(jnp.logical_not(is_first))
        def _():
            backward_copy(m).wait_send()

        return carry

    lax.fori_loop(0, micro_count, drain, 0)


def run_pipeline(inside, patches, cotangent, embed, live, hidden_mask, width_inv, gain, w_up, w_down):
    section_count = lax.axis_size("section")
    shard_count = lax.axis_size("fsdp")
    micro_count, rows, features = patches.shape
    hidden_count = w_up.shape[1]
    vmem = pl.BlockSpec(memory_space=pltpu.VMEM)
    token = (micro_count, rows, features)
    tokens = micro_count * rows
    chips = shard_count // 2
    dma = pltpu.SemaphoreType.DMA
    scratch = [
        pltpu.VMEM(token, BF16),
        pltpu.VMEM(token, BF16),
        pltpu.VMEM(token, BF16),
        pltpu.VMEM(token, BF16),
        pltpu.VMEM((tokens, hidden_count), BF16),
        pltpu.VMEM((tokens, hidden_count), BF16),
        pltpu.VMEM((features, tokens), BF16),
        pltpu.VMEM((features, tokens), BF16),
        dma((micro_count,)),
        dma((micro_count,)),
        dma((micro_count,)),
        dma((micro_count,)),
    ]
    if inside:
        up_rows, down_rows = features // shard_count, hidden_count // shard_count
        scratch += [
            pltpu.VMEM((features, hidden_count), BF16),
            pltpu.VMEM((hidden_count, features), BF16),
            pltpu.VMEM((shard_count, 8, features), F32),
            pltpu.VMEM((shard_count, 8, features), F32),
            pltpu.VMEM((8, features), F32),
            pltpu.VMEM((chips, up_rows, hidden_count), BF16),
            pltpu.VMEM((chips, down_rows, features), BF16),
            pltpu.VMEM((chips + 1, up_rows, hidden_count), BF16),
            pltpu.VMEM((chips + 1, down_rows, features), BF16),
            dma((4, 2, chips)),
            dma((4, chips)),
            dma((4, chips)),
            dma((4, chips)),
            dma((2, chips)),
            dma((2, chips + 1)),
            dma((2, chips)),
            dma((2, chips)),
        ]
        grads = (
            jax.ShapeDtypeStruct((up_rows, hidden_count), F32),
            jax.ShapeDtypeStruct((down_rows, features), F32),
        )
    else:
        grads = (
            jax.ShapeDtypeStruct((features, hidden_count), BF16),
            jax.ShapeDtypeStruct((hidden_count, features), BF16),
        )
    return pl.pallas_call(
        functools.partial(pipeline_kernel, section_count, shard_count),
        out_shape=grads + (jax.ShapeDtypeStruct((8, features), F32),),
        in_specs=[vmem] * 9,
        out_specs=(vmem, vmem, vmem),
        scratch_shapes=scratch,
        compiler_params=pltpu.CompilerParams(
            collective_id=0, has_side_effects=True, vmem_limit_bytes=VMEM_BYTES
        ),
    )(patches, cotangent, embed, live, hidden_mask, width_inv, gain, w_up, w_down)


def per_device(patches, cotangent, embed_blocks, ratio_index, depth, w_up, w_down, ln_gain):
    section_index = lax.axis_index("section")
    shard_index = lax.axis_index("fsdp")
    shard_count = lax.axis_size("fsdp")
    micro_count, rows, features = patches.shape
    hidden_count = w_up.shape[2]
    gain_count = ln_gain.shape[1]
    tiled = gain_count % 16 == 0 and w_down.shape[1] % 128 == 0 and shard_count % 2 == 0

    width = embed_blocks * BLOCK
    hidden_width = width * (6 + ratio_index) // 2
    embed = (lax.iota(jnp.int32, features)[None, :] < width[:, None]).astype(F32)
    hidden_mask = (lax.iota(jnp.int32, hidden_count)[None, :] < hidden_width[:, None]).astype(F32)
    active = (section_index < depth).astype(F32)
    live = embed * active[:, None]
    width_inv = jnp.broadcast_to((1.0 / width.astype(F32))[:, None, None], (micro_count, 1, BLOCK))
    masks = (embed[:, None, :], live[:, None, :], hidden_mask[:, None, :], width_inv)
    start = shard_index * gain_count

    if tiled:
        gain = jnp.zeros((8, features), F32)
        gain = lax.dynamic_update_slice(gain, ln_gain.astype(F32), (jnp.int32(0), start))
        own_up, own_down, gains = run_pipeline(
            True, patches, cotangent, *masks, gain, w_up[0], w_down[0]
        )
        own_gain = lax.dynamic_slice(jnp.sum(gains, axis=0), (start,), (gain_count,))
        return (own_up[None], own_down[None], own_gain[None])

    full_up = lax.all_gather(w_up[0], "fsdp", axis=0, tiled=True)
    full_down = lax.all_gather(w_down[0], "fsdp", axis=0, tiled=True)
    gain = lax.all_gather(ln_gain[0], "fsdp", axis=0, tiled=True).astype(F32)
    gain = jnp.broadcast_to(gain[None], (8, features))
    part_up, part_down, gains = run_pipeline(
        False, patches, cotangent, *masks, gain, full_up, full_down
    )
    own_down = lax.psum_scatter(part_down, "fsdp", scatter_dimension=0, tiled=True)
    own_up = lax.psum_scatter(part_up, "fsdp", scatter_dimension=0, tiled=True)
    part_gain = jnp.sum(gains, axis=0)
    own_gain = lax.psum_scatter(part_gain, "fsdp", scatter_dimension=0, tiled=True)
    return (own_up.astype(F32)[None], own_down.astype(F32)[None], own_gain[None])


def solution(mesh):
    return jax.shard_map(
        per_device,
        mesh=mesh,
        in_specs=(
            P(None, "fsdp", None),
            P(None, "fsdp", None),
            P(),
            P(),
            P(),
            P("section", "fsdp", None),
            P("section", "fsdp", None),
            P("section", "fsdp"),
        ),
        out_specs=(P("section", "fsdp", None), P("section", "fsdp", None), P("section", "fsdp")),
        check_vma=False,
    )
```

```python
import functools
import math

import jax
import jax.numpy as jnp
from jax import lax
from jax.experimental import pallas as pl
from jax.experimental.pallas import tpu as pltpu
from jax.sharding import PartitionSpec as P

BLOCK = 128
EPSILON = 1e-05
SCALE = 0.7978845608028654
MESH = pl.DeviceIdType.MESH
VMEM_BYTES = 66 * 1024 * 1000
BF16 = jnp.bfloat16
F32 = jnp.float32


def gelu_and_slope(hidden):
    square = hidden * hidden
    tanh = jnp.tanh(hidden * (SCALE + (SCALE * 0.044715) * square))
    half = 0.5 + 0.5 * tanh
    rise = (hidden * (0.5 * SCALE + (0.5 * SCALE * 0.134145) * square)) * (1.0 - tanh * tanh)
    return (hidden * half, half + rise)


def contract_last(left, right):
    return lax.dot_general(left, right, (((1,), (1,)), ((), ())), preferred_element_type=F32)


def chunks(total, size):
    size = size if total % size == 0 else total
    return [(start, size) for start in range(0, total, size)]


def signal(semaphore, device):
    pl.semaphore_signal(semaphore, inc=1, device_id=device, device_id_type=MESH)


def pipeline_kernel(
    section_count,
    shard_count,
    patches,
    cotangent,
    embed,
    live,
    hidden_mask,
    width_inv,
    own_gain,
    own_up,
    own_down,
    grad_up,
    grad_down,
    grad_gain,
    x_in,
    x_out,
    g_in,
    g_out,
    act,
    slope,
    normed_t,
    branch_t,
    fwd_send,
    fwd_recv,
    bwd_send,
    bwd_recv,
    w_up=None,
    w_down=None,
    hold_up=None,
    hold_down=None,
    all_gain=None,
    all_rise=None,
    acc_gain=None,
    pair_up=None,
    pair_down=None,
    first_up=None,
    first_down=None,
    second_up=None,
    second_down=None,
    plane_up=None,
    plane_down=None,
    last_up=None,
    last_down=None,
    token_send=None,
    token_recv=None,
    gain_send=None,
    gain_recv=None,
    scatter_send=None,
    scatter_recv=None,
    climb_send=None,
    climb_recv=None,
    side_send=None,
    side_recv=None,
    pair_send=None,
    pair_recv=None,
    sum_pair_send=None,
    sum_pair_recv=None,
    first_send=None,
    first_recv=None,
    second_send=None,
    second_recv=None,
    plane_send=None,
    plane_recv=None,
    last_send=None,
    last_recv=None,
):
    planes = w_up is not None
    column = lax.axis_index("section")
    shard = lax.axis_index("fsdp")
    chip = shard // 2
    core = shard % 2
    chips = shard_count // 2
    me = chip if planes else column
    stages = chips if planes else section_count
    is_first = me == 0
    is_last = me == stages - 1
    micro_count, rows, features = patches.shape
    hidden_count = hidden_mask.shape[2]

    def stage_device(stage):
        return {"fsdp": 2 * stage + core} if planes else {"section": stage}

    barrier = pltpu.get_barrier_semaphore()
    if planes:
        for column_to in range(section_count):
            for shard_to in range(shard_count):

                @pl.when(jnp.logical_or(column != column_to, shard != shard_to))
                def _():
                    signal(barrier, {"section": column_to, "fsdp": shard_to})

        pl.semaphore_wait(barrier, section_count * shard_count - 1)
    else:

        @pl.when(jnp.logical_not(is_first))
        def _():
            signal(barrier, {"section": me - 1})

        @pl.when(jnp.logical_not(is_last))
        def _():
            signal(barrier, {"section": me + 1})

        pl.semaphore_wait(barrier, 2 - is_first.astype(jnp.int32) - is_last.astype(jnp.int32))

    def remote(source, target, send, recv, device):
        return pltpu.make_async_remote_copy(
            src_ref=source,
            dst_ref=target,
            send_sem=send,
            recv_sem=recv,
            device_id=device,
            device_id_type=MESH,
        )

    if planes:
        beside = column + 1 - 2 * (column % 2)
        across = column + 2 - 4 * (column // 2)
        corner = 3 - column
        near = (column, beside, across, corner)
        other = {"fsdp": shard + 1 - 2 * core}
        up_rows, down_rows = features // shard_count, hidden_count // shard_count
        up_cols, down_part = hidden_count // section_count, down_rows // section_count
        share = rows // section_count

        def at_rows(start, size):
            return pl.ds(pl.multiple_of(start, size), size)

        def piece(number, full, place, which):
            if number == 0:
                return full.at[at_rows((2 * place + core) * up_rows, up_rows), at_rows(which * up_cols, up_cols)]
            return full.at[at_rows(((2 * place + core) * section_count + which) * down_part, down_part), :]

        def own_piece(number, which):
            if number == 0:
                return own_up.at[:, at_rows(which * up_cols, up_cols)]
            return own_down.at[at_rows(which * down_part, down_part), :]

        fulls = (w_up, w_down)
        holds = (hold_up, hold_down)

        def token_copy(number, m, source):
            raw, land, stage = ((patches, x_in, 0), (cotangent, g_in, stages - 1))[number]
            return remote(
                raw.at[m, at_rows(column * share, share), :],
                land.at[m, at_rows(source * share, share), :],
                token_send.at[number, m],
                token_recv.at[number, m, source],
                stage_device(stage),
            )

        def send_tokens(number, first, last):
            raw, land, stage = ((patches, x_in, 0), (cotangent, g_in, stages - 1))[number]

            @pl.when(chip != stage)
            def _():
                for m in range(first, last):
                    token_copy(number, m, chip).start()

            @pl.when(chip == stage)
            def _():
                for m in range(first, last):
                    land[m, at_rows(chip * share, share), :] = raw[m, at_rows(column * share, share), :]

        def wait_tokens(number, m):
            for source in range(chips):

                @pl.when(chip != source)
                def _():
                    token_copy(number, m, source).wait_recv()

        def scatter_copy(number, far):
            return remote(
                own_piece(number, near[far]),
                holds[number].at[column],
                scatter_send.at[number, far - 1],
                scatter_recv.at[number, column],
                {"section": near[far]},
            )

        def scatter_wait(number, source):
            hold = holds[number]
            remote(
                hold.at[source],
                hold.at[source],
                scatter_send.at[number, 0],
                scatter_recv.at[number, source],
                {"section": beside},
            ).wait_recv()

        def climb_copy(number, source, layer, place):
            return remote(
                source,
                piece(number, fulls[number], place, column),
                climb_send.at[number, layer],
                climb_recv.at[number, place],
                {"fsdp": 2 * layer + core},
            )

        def side_copy(number, way, place, which, kind, device):
            spot = piece(number, fulls[number], place, which)
            return remote(
                spot,
                spot,
                side_send.at[number, way, place],
                side_recv.at[number, kind, place],
                {"section": device},
            )

        def to_beside(number, place):
            return side_copy(number, 0, place, column, 0, beside)

        def to_across(number, place):
            return side_copy(number, 1, place, column, 1, across)

        def relay(number, place):
            if number == 0:
                return side_copy(number, 2, place, beside, 2, across)
            return side_copy(number, 2, place, across, 2, beside)

        def arrived(number, place, kind):
            side_copy(number, 0, place, near[kind + 1], kind, beside).wait_recv()

        def pair_copy(number, place, far, parity):
            which = near[far]
            full = fulls[number]
            if number == 0:
                spot = full.at[at_rows((2 * place + parity) * up_rows, up_rows), at_rows(which * up_cols, up_cols)]
            else:
                first = ((2 * place + parity) * section_count + which) * down_part
                spot = full.at[at_rows(first, down_part), :]
            return remote(
                spot, spot, pair_send.at[number, far, place], pair_recv.at[number, far, place], other
            )

        def gain_targets(number):
            if number == 0:
                return [(j, 2 * column + half, 2 * j + half) for j in range(section_count) for half in range(2)]
            return [(chip, place, place) for place in range(shard_count)]

        def open_gain(block, land, number):
            source = shard if number == 0 else 2 * column + core
            for column_to, shard_to, index in gain_targets(number):
                copy = remote(
                    block,
                    land.at[source],
                    gain_send.at[number, index],
                    gain_recv.at[number, source],
                    {"section": column_to, "fsdp": shard_to},
                )

                @pl.when(jnp.logical_or(column_to != column, shard_to != shard))
                def _():
                    copy.start()

            @pl.when(chip == column)
            def _():
                land[source] = block[...]

        def close_gain(block, land, number):
            mine = shard if number == 0 else 2 * column + core
            for source in range(shard_count):

                @pl.when(jnp.logical_or(chip != column, source != mine))
                def _():
                    remote(
                        block, land.at[source], gain_send.at[number, 0], gain_recv.at[number, source], other
                    ).wait_recv()

        def sent_gain(block, land, number):
            for column_to, shard_to, index in gain_targets(number):

                @pl.when(jnp.logical_or(column_to != column, shard_to != shard))
                def _():
                    remote(
                        block, land.at[0], gain_send.at[number, index], gain_recv.at[number, 0], other
                    ).wait_send()

        both = (0, 1)
        for number in both:
            for far in (1, 2, 3):
                scatter_copy(number, far).start()
        send_tokens(0, 0, 1)
        open_gain(own_gain, all_gain, 0)
        for far in (0, 1, 2, 3):
            layer = near[far]
            for number in both:
                if far == 0:
                    source = own_piece(number, column)
                else:
                    scatter_wait(number, layer)
                    source = holds[number].at[layer]

                @pl.when(layer != chip)
                def _():
                    climb_copy(number, source, layer, chip).start()

                @pl.when(layer == chip)
                def _():
                    spot = piece(number, fulls[number], chip, column)
                    spot[...] = source[...]

        send_tokens(0, 1, micro_count)
        send_tokens(1, 0, micro_count)

        def own_turn(step):
            place = lax.rem(chip + step, chips)
            for number in both:
                if step > 0:
                    spot = piece(number, fulls[number], place, column)
                    climb_copy(number, spot, chip, place).wait_recv()
                to_beside(number, place).start()
                to_across(number, place).start()
                pair_copy(number, place, 0, core).start()

        def side_turn(step):
            place = lax.rem(chip + step, chips)
            arrived(0, place, 0)
            relay(0, place).start()
            pair_copy(0, place, 1, core).start()
            arrived(1, place, 1)
            relay(1, place).start()
            pair_copy(1, place, 2, core).start()
            arrived(0, place, 1)
            pair_copy(0, place, 2, core).start()
            arrived(1, place, 0)
            pair_copy(1, place, 1, core).start()

        def corner_turn(step):
            place = lax.rem(chip + step, chips)
            for number in both:
                arrived(number, place, 2)
                pair_copy(number, place, 3, core).start()

        for step in range(chips + 2):
            if step < chips:
                own_turn(step)
            if 1 <= step <= chips:
                side_turn(step - 1)
            if 2 <= step:
                corner_turn(step - 2)
        for place in range(chips):
            for far in (0, 1, 2, 3):
                for number in both:
                    pair_copy(number, place, far, 1 - core).wait_recv()
        close_gain(own_gain, all_gain, 0)
        gain = jnp.sum(all_gain[...], axis=0)[:1]
    else:
        w_up, w_down, acc_gain = own_up, own_down, grad_gain
        gain = own_gain[:1]

    def forward_copy(m):
        return pltpu.make_async_remote_copy(
            src_ref=x_out.at[m],
            dst_ref=x_in.at[m],
            send_sem=fwd_send.at[m],
            recv_sem=fwd_recv.at[m],
            device_id=stage_device(jnp.minimum(me + 1, stages - 1)),
            device_id_type=MESH,
        )

    def backward_copy(m):
        return pltpu.make_async_remote_copy(
            src_ref=g_out.at[m],
            dst_ref=g_in.at[m],
            send_sem=bwd_send.at[m],
            recv_sem=bwd_recv.at[m],
            device_id=stage_device(jnp.maximum(me - 1, 0)),
            device_id_type=MESH,
        )

    def layer_norm(m):
        mask = embed[m]
        scale = width_inv[m][:, :1]
        values = x_in[m].astype(F32) * mask
        center = jnp.sum(values, axis=-1, keepdims=True) * scale
        centered = (values - center) * mask
        variance = jnp.sum(centered * centered, axis=-1, keepdims=True) * scale
        inv_std = lax.rsqrt(variance + EPSILON)
        return centered * inv_std, inv_std

    def forward(m, carry):
        at = pl.ds(pl.multiple_of(m * rows, rows), rows)

        @pl.when(is_first)
        def _():
            if planes:
                wait_tokens(0, m)
                x_in[m] = (x_in[m].astype(F32) * embed[m]).astype(BF16)
            else:
                x_in[m] = (patches[m].astype(F32) * embed[m]).astype(BF16)

        @pl.when(jnp.logical_not(is_first))
        def _():
            forward_copy(m).wait_recv()

        standard, _ = layer_norm(m)
        scaled = standard * gain
        normed = scaled.astype(BF16)
        normed_t[:, at] = jnp.transpose(scaled).astype(BF16)
        for start, size in chunks(hidden_count, 512):
            part = pl.ds(start, size)
            hidden = jnp.dot(normed, w_up[:, part], preferred_element_type=F32)
            value, rise = gelu_and_slope(hidden)
            mask = hidden_mask[m, :, part]
            act[at, part] = (value * mask).astype(BF16)
            slope[at, part] = (rise * mask).astype(BF16)

        @pl.when(jnp.logical_not(is_last))
        def _():
            for start, size in chunks(features, 256):
                part = pl.ds(start, size)
                branch = jnp.dot(act[at, :], w_down[:, part], preferred_element_type=F32)
                out = x_in[m, :, part].astype(F32) + live[m, :, part] * branch
                x_out[m, :, part] = out.astype(BF16)
            forward_copy(m).start()

        return carry

    lax.fori_loop(0, micro_count, forward, 0)
    acc_gain[...] = jnp.zeros_like(acc_gain)

    def backward(m, carry):
        at = pl.ds(pl.multiple_of(m * rows, rows), rows)

        @pl.when(is_last)
        def _():
            if planes:
                wait_tokens(1, m)
                g_in[m] = (g_in[m].astype(F32) * embed[m]).astype(BF16)
            else:
                g_in[m] = (cotangent[m].astype(F32) * embed[m]).astype(BF16)

        @pl.when(jnp.logical_not(is_last))
        def _():
            backward_copy(m).wait_recv()

        grad_float = g_in[m].astype(F32)
        branch_float = grad_float * live[m]
        branch = branch_float.astype(BF16)
        branch_t[:, at] = jnp.transpose(branch_float).astype(BF16)
        for start, size in chunks(hidden_count, 512):
            part = pl.ds(start, size)
            grad_act = contract_last(branch, w_down[part, :])
            slope[at, part] = (grad_act * slope[at, part].astype(F32)).astype(BF16)
        grad_hidden = slope[at, :]
        grad_normed = jnp.concatenate(
            [
                contract_last(grad_hidden, w_up[pl.ds(start, size), :])
                for start, size in chunks(features, 256)
            ],
            axis=1,
        )
        standard, inv_std = layer_norm(m)
        mask = embed[m]
        scale = width_inv[m][:, :1]
        acc_gain[...] += jnp.sum((grad_normed * standard).reshape(-1, 8, features), axis=0)

        @pl.when(jnp.logical_not(is_first))
        def _():
            grad_standard = grad_normed * gain * mask
            first = jnp.sum(grad_standard, axis=-1, keepdims=True) * scale
            second = jnp.sum(grad_standard * standard, axis=-1, keepdims=True) * scale
            grad_x = inv_std * (grad_standard - first * mask - standard * second)
            g_out[m] = (grad_float + grad_x).astype(BF16)
            backward_copy(m).start()

        return carry

    lax.fori_loop(0, micro_count, backward, 0)

    width = 256 if hidden_count % 256 == 0 else hidden_count

    def up_grads(first, size, step):
        part = pl.ds(pl.multiple_of(step * width, width), width)
        these = pl.ds(first, size)
        return these, part, jnp.dot(normed_t[these, :], slope[:, part], preferred_element_type=F32)

    def down_grads(part):
        down = jnp.dot(branch_t[...], act[:, part], preferred_element_type=F32)
        return jnp.transpose(down).astype(BF16)

    def weight_grads(step, carry):
        these, part, up = up_grads(0, features, step)
        grad_up[these, part] = up.astype(BF16)
        grad_down[part, :] = down_grads(part)
        return carry

    def slot(full, index):
        size = full.shape[0] // shard_count
        return full.at[pl.ds(pl.multiple_of(index * size, size), size)]

    if planes:
        pairs = (pair_up, pair_down)
        firsts = (first_up, first_down)
        seconds = (second_up, second_down)
        finals = (plane_up, plane_down)
        lasts = (last_up, last_down)
        first_way = (beside, across)
        second_way = (across, beside)
        kept = (across, beside)

        def sum_pair(number, place):
            return remote(
                slot(fulls[number], 2 * place + 1 - core),
                pairs[number].at[place],
                sum_pair_send.at[number, place],
                sum_pair_recv.at[number, place],
                other,
            )

        def first_copy(number, place, index):
            which = (first_way[number], corner)[index]
            return remote(
                piece(number, fulls[number], place, which),
                firsts[number].at[place, index],
                first_send.at[number, place, index],
                first_recv.at[number, place, index],
                {"section": first_way[number]},
            )

        def second_copy(number, place):
            return remote(
                piece(number, fulls[number], place, kept[number]),
                seconds[number].at[place],
                second_send.at[number, place],
                second_recv.at[number, place],
                {"section": second_way[number]},
            )

        def plane_copy(number, place, layer):
            return remote(
                piece(number, fulls[number], place, column),
                finals[number].at[layer],
                plane_send.at[number, place],
                plane_recv.at[number, layer],
                {"fsdp": 2 * place + core},
            )

        def last_copy(number, layer, source):
            return remote(
                finals[number].at[layer],
                lasts[number].at[source],
                last_send.at[number, layer],
                last_recv.at[number, source],
                {"section": layer},
            )

        def make_grads(place):
            up_size = 2 * up_rows
            first_row = pl.multiple_of(place * up_size, up_size)

            def up_step(step, carry):
                these, part, up = up_grads(first_row, up_size, step)
                w_up[these, part] = up.astype(BF16)
                return carry

            lax.fori_loop(0, hidden_count // width, up_step, 0)
            sum_pair(0, place).start()
            down_size = 2 * down_rows
            size = math.gcd(down_size, width)

            def down_step(step, carry):
                part = at_rows(place * down_size + step * size, size)
                w_down[part, :] = down_grads(part)
                return carry

            lax.fori_loop(0, down_size // size, down_step, 0)
            sum_pair(1, place).start()

        def first_turn(place):
            for number in both:
                mine = slot(fulls[number], 2 * place + core)
                sum_pair(number, place).wait_recv()
                mine[...] = (mine[...].astype(F32) + pairs[number][place].astype(F32)).astype(BF16)
                for index in (0, 1):
                    first_copy(number, place, index).start()

        def second_turn(place):
            for number in both:
                for index in (1, 0):
                    first_copy(number, place, index).wait_recv()
                spot = piece(number, fulls[number], place, kept[number])
                total = spot[...].astype(F32) + firsts[number][place, 1].astype(F32)
                spot[...] = total.astype(BF16)
                second_copy(number, place).start()

        def plane_turn(place):
            for number in both:
                second_copy(number, place).wait_recv()
                spot = piece(number, fulls[number], place, column)
                total = spot[...].astype(F32) + firsts[number][place, 0].astype(F32)
                total = (total + seconds[number][place].astype(F32)).astype(BF16)

                @pl.when(place != chip)
                def _():
                    spot[...] = total
                    plane_copy(number, place, chip).start()

                @pl.when(place == chip)
                def _():
                    finals[number][chip] = total

        def place_at(index):
            return lax.rem(chip + chips - 1 - index + chips, chips)

        def reduce_step(index, carry):
            @pl.when(index < chips)
            def _():
                make_grads(place_at(index))
                first_turn(place_at(index))

            @pl.when(jnp.logical_and(index >= 1, index <= chips))
            def _():
                second_turn(place_at(jnp.maximum(index - 1, 0)))

            @pl.when(index >= 2)
            def _():
                plane_turn(place_at(jnp.maximum(index - 2, 0)))

            return carry

        open_gain(acc_gain, all_rise, 1)
        for number in both:
            for far in (1, 2, 3):
                scatter_copy(number, far).wait_send()
            for layer in range(chips):

                @pl.when(chip != layer)
                def _():
                    climb_copy(number, holds[number].at[layer], layer, chip).wait_send()

            for place in range(chips):
                to_beside(number, place).wait_send()
                to_across(number, place).wait_send()
                relay(number, place).wait_send()
                for far in (0, 1, 2, 3):
                    pair_copy(number, place, far, core).wait_send()
        sent_gain(own_gain, all_gain, 0)
        lax.fori_loop(0, chips + 2, reduce_step, 0)
        for layer in reversed(range(chips)):
            for number in both:

                @pl.when(layer != chip)
                def _():
                    plane_copy(number, chip, layer).wait_recv()

                @pl.when(layer != column)
                def _():
                    last_copy(number, layer, column).start()

                @pl.when(layer == column)
                def _():
                    lasts[number][layer] = finals[number][layer]

        close_gain(acc_gain, all_rise, 1)
        grad_gain[...] = jnp.sum(all_rise[...], axis=0)
        for source in range(section_count):
            for number in both:

                @pl.when(source != column)
                def _():
                    last_copy(number, source, source).wait_recv()

            grad_up[:, pl.ds(source * up_cols, up_cols)] = last_up[source].astype(F32)
            grad_down[pl.ds(source * down_part, down_part), :] = last_down[source].astype(F32)
        sent_gain(acc_gain, all_rise, 1)
        for number in both:
            for place in range(chips):
                sum_pair(number, place).wait_send()
                second_copy(number, place).wait_send()
                for index in (0, 1):
                    first_copy(number, place, index).wait_send()

                @pl.when(place != chip)
                def _():
                    plane_copy(number, place, chip).wait_send()

                @pl.when(place != column)
                def _():
                    last_copy(number, place, column).wait_send()

        for number, stage in ((0, 0), (1, stages - 1)):

            @pl.when(chip != stage)
            def _():
                for m in range(micro_count):
                    token_copy(number, m, chip).wait_send()
    else:
        lax.fori_loop(0, hidden_count // width, weight_grads, 0)

    def drain(m, carry):
        @pl.when(jnp.logical_not(is_last))
        def _():
            forward_copy(m).wait_send()

        @pl.when(jnp.logical_not(is_first))
        def _():
            backward_copy(m).wait_send()

        return carry

    lax.fori_loop(0, micro_count, drain, 0)


def run_pipeline(planes, patches, cotangent, embed, live, hidden_mask, width_inv, gain, w_up, w_down):
    section_count = lax.axis_size("section")
    shard_count = lax.axis_size("fsdp")
    micro_count, rows, features = patches.shape
    hidden_count = w_up.shape[1]
    vmem = pl.BlockSpec(memory_space=pltpu.VMEM)
    token = (micro_count, rows, features)
    tokens = micro_count * rows
    chips = shard_count // 2
    dma = pltpu.SemaphoreType.DMA
    scratch = [
        pltpu.VMEM(token, BF16),
        pltpu.VMEM(token, BF16),
        pltpu.VMEM(token, BF16),
        pltpu.VMEM(token, BF16),
        pltpu.VMEM((tokens, hidden_count), BF16),
        pltpu.VMEM((tokens, hidden_count), BF16),
        pltpu.VMEM((features, tokens), BF16),
        pltpu.VMEM((features, tokens), BF16),
        dma((micro_count,)),
        dma((micro_count,)),
        dma((micro_count,)),
        dma((micro_count,)),
    ]
    if planes:
        up_rows, down_rows = features // shard_count, hidden_count // shard_count
        up_piece = (up_rows, hidden_count // section_count)
        down_piece = (down_rows // section_count, features)
        scratch += [
            pltpu.VMEM((features, hidden_count), BF16),
            pltpu.VMEM((hidden_count, features), BF16),
            pltpu.VMEM((section_count,) + up_piece, BF16),
            pltpu.VMEM((section_count,) + down_piece, BF16),
            pltpu.VMEM((shard_count, 8, features), F32),
            pltpu.VMEM((shard_count, 8, features), F32),
            pltpu.VMEM((8, features), F32),
            pltpu.VMEM((chips, up_rows, hidden_count), BF16),
            pltpu.VMEM((chips, down_rows, features), BF16),
            pltpu.VMEM((chips, 2) + up_piece, BF16),
            pltpu.VMEM((chips, 2) + down_piece, BF16),
            pltpu.VMEM((chips,) + up_piece, BF16),
            pltpu.VMEM((chips,) + down_piece, BF16),
            pltpu.VMEM((chips,) + up_piece, BF16),
            pltpu.VMEM((chips,) + down_piece, BF16),
            pltpu.VMEM((section_count,) + up_piece, BF16),
            pltpu.VMEM((section_count,) + down_piece, BF16),
            dma((2, micro_count)),
            dma((2, micro_count, chips)),
            dma((2, shard_count)),
            dma((2, shard_count)),
            dma((2, 3)),
            dma((2, section_count)),
            dma((2, chips)),
            dma((2, chips)),
            dma((2, 3, chips)),
            dma((2, 3, chips)),
            dma((2, 4, chips)),
            dma((2, 4, chips)),
            dma((2, chips)),
            dma((2, chips)),
            dma((2, chips, 2)),
            dma((2, chips, 2)),
            dma((2, chips)),
            dma((2, chips)),
            dma((2, chips)),
            dma((2, chips)),
            dma((2, chips)),
            dma((2, section_count)),
        ]
        grads = (
            jax.ShapeDtypeStruct((up_rows, hidden_count), F32),
            jax.ShapeDtypeStruct((down_rows, features), F32),
        )
    else:
        grads = (
            jax.ShapeDtypeStruct((features, hidden_count), BF16),
            jax.ShapeDtypeStruct((hidden_count, features), BF16),
        )
    return pl.pallas_call(
        functools.partial(pipeline_kernel, section_count, shard_count),
        out_shape=grads + (jax.ShapeDtypeStruct((8, features), F32),),
        in_specs=[vmem] * 9,
        out_specs=(vmem, vmem, vmem),
        scratch_shapes=scratch,
        compiler_params=pltpu.CompilerParams(
            collective_id=0, has_side_effects=True, vmem_limit_bytes=VMEM_BYTES
        ),
    )(patches, cotangent, embed, live, hidden_mask, width_inv, gain, w_up, w_down)


def per_device(patches, cotangent, embed_blocks, ratio_index, depth, w_up, w_down, ln_gain):
    section_index = lax.axis_index("section")
    shard_index = lax.axis_index("fsdp")
    shard_count = lax.axis_size("fsdp")
    micro_count, rows, features = patches.shape
    hidden_count = w_up.shape[2]
    gain_count = ln_gain.shape[1]
    section_count = lax.axis_size("section")
    down_part = w_down.shape[1] // section_count
    planes = (
        section_count == 4
        and shard_count == 2 * section_count
        and gain_count % 16 == 0
        and down_part % 16 == 0
        and hidden_count % (128 * section_count) == 0
        and rows % (16 * section_count) == 0
    )

    width = embed_blocks * BLOCK
    hidden_width = width * (6 + ratio_index) // 2
    embed = (lax.iota(jnp.int32, features)[None, :] < width[:, None]).astype(F32)
    hidden_mask = (lax.iota(jnp.int32, hidden_count)[None, :] < hidden_width[:, None]).astype(F32)
    layer = shard_index // 2 if planes else section_index
    active = (layer < depth).astype(F32)
    live = embed * active[:, None]
    width_inv = jnp.broadcast_to((1.0 / width.astype(F32))[:, None, None], (micro_count, 1, BLOCK))
    masks = (embed[:, None, :], live[:, None, :], hidden_mask[:, None, :], width_inv)
    start = shard_index * gain_count

    if planes:
        gain = jnp.zeros((8, features), F32)
        gain = lax.dynamic_update_slice(gain, ln_gain.astype(F32), (jnp.int32(0), start))
        own_up, own_down, gains = run_pipeline(
            True, patches, cotangent, *masks, gain, w_up[0], w_down[0]
        )
        own_gain = lax.dynamic_slice(jnp.sum(gains, axis=0), (start,), (gain_count,))
        return (own_up[None], own_down[None], own_gain[None])

    full_up = lax.all_gather(w_up[0], "fsdp", axis=0, tiled=True)
    full_down = lax.all_gather(w_down[0], "fsdp", axis=0, tiled=True)
    gain = lax.all_gather(ln_gain[0], "fsdp", axis=0, tiled=True).astype(F32)
    gain = jnp.broadcast_to(gain[None], (8, features))
    part_up, part_down, gains = run_pipeline(
        False, patches, cotangent, *masks, gain, full_up, full_down
    )
    own_down = lax.psum_scatter(part_down, "fsdp", scatter_dimension=0, tiled=True)
    own_up = lax.psum_scatter(part_up, "fsdp", scatter_dimension=0, tiled=True)
    part_gain = jnp.sum(gains, axis=0)
    own_gain = lax.psum_scatter(part_gain, "fsdp", scatter_dimension=0, tiled=True)
    return (own_up.astype(F32)[None], own_down.astype(F32)[None], own_gain[None])


def solution(mesh):
    return jax.shard_map(
        per_device,
        mesh=mesh,
        in_specs=(
            P(None, "fsdp", None),
            P(None, "fsdp", None),
            P(),
            P(),
            P(),
            P("section", "fsdp", None),
            P("section", "fsdp", None),
            P("section", "fsdp"),
        ),
        out_specs=(P("section", "fsdp", None), P("section", "fsdp", None), P("section", "fsdp")),
        check_vma=False,
    )
```

```python
import functools
import math

import jax
import jax.numpy as jnp
from jax import lax
from jax.experimental import pallas as pl
from jax.experimental.pallas import tpu as pltpu
from jax.sharding import PartitionSpec as P

BLOCK = 128
SPLIT = False
EPSILON = 1e-05
SCALE = 0.7978845608028654
MESH = pl.DeviceIdType.MESH
VMEM_BYTES = 66 * 1024 * 1000
BF16 = jnp.bfloat16
F32 = jnp.float32


def gelu_and_slope(hidden):
    square = hidden * hidden
    tanh = jnp.tanh(hidden * (SCALE + (SCALE * 0.044715) * square))
    half = 0.5 + 0.5 * tanh
    rise = (hidden * (0.5 * SCALE + (0.5 * SCALE * 0.134145) * square)) * (1.0 - tanh * tanh)
    return (hidden * half, half + rise)


def contract_last(left, right):
    return lax.dot_general(left, right, (((1,), (1,)), ((), ())), preferred_element_type=F32)


def chunks(total, size):
    size = size if total % size == 0 else total
    return [(start, size) for start in range(0, total, size)]


def signal(semaphore, device):
    pl.semaphore_signal(semaphore, inc=1, device_id=device, device_id_type=MESH)


def pipeline_kernel(
    section_count,
    shard_count,
    patches,
    cotangent,
    table,
    own_gain,
    own_up,
    own_down,
    grad_up,
    grad_down,
    grad_gain,
    x_in,
    x_out,
    g_in,
    g_out,
    act,
    slope,
    normed_t,
    branch_t,
    fwd_send,
    fwd_recv,
    bwd_send,
    bwd_recv,
    w_up=None,
    w_down=None,
    hold_up=None,
    hold_down=None,
    all_gain=None,
    all_rise=None,
    rise_own=None,
    rise_sum=None,
    acc_gain=None,
    pair_up=None,
    pair_down=None,
    first_up=None,
    first_down=None,
    second_up=None,
    second_down=None,
    plane_up=None,
    plane_down=None,
    last_up=None,
    last_down=None,
    token_send=None,
    token_recv=None,
    gain_send=None,
    gain_recv=None,
    rise_send=None,
    rise_recv=None,
    scatter_send=None,
    scatter_recv=None,
    climb_send=None,
    climb_recv=None,
    side_send=None,
    side_recv=None,
    pair_send=None,
    pair_recv=None,
    sum_pair_send=None,
    sum_pair_recv=None,
    first_send=None,
    first_recv=None,
    second_send=None,
    second_recv=None,
    plane_send=None,
    plane_recv=None,
    last_send=None,
    last_recv=None,
):
    planes = w_up is not None
    column = lax.axis_index("section")
    shard = lax.axis_index("fsdp")
    chip = shard // 2
    core = shard % 2
    chips = shard_count // 2
    me = chip if planes else column
    stages = chips if planes else section_count
    is_first = me == 0
    is_last = me == stages - 1
    micro_count, rows, features = patches.shape
    hidden_count = table.shape[2]
    features_all = pl.ds(0, features)
    halves = micro_count // table.shape[0]

    def hidden_mask(m, part):
        return table[m // halves, 0:1, part]

    def embed(m, part=features_all):
        return table[m // halves, 1:2, part]

    def live(m, part=features_all):
        return table[m // halves, 2:3, part]

    def width_inv(m):
        return table[m // halves, 3:4, 0:1]

    def stage_device(stage):
        return {"fsdp": 2 * stage + core} if planes else {"section": stage}

    barrier = pltpu.get_barrier_semaphore()
    if planes:
        for step in range(1, section_count):
            signal(barrier, {"section": lax.rem(column + step, section_count)})
            signal(barrier, {"fsdp": lax.rem(shard + 2 * step, shard_count)})
        signal(barrier, {"fsdp": shard + 1 - 2 * core})
        pl.semaphore_wait(barrier, 2 * section_count - 1)
    else:

        @pl.when(jnp.logical_not(is_first))
        def _():
            signal(barrier, {"section": me - 1})

        @pl.when(jnp.logical_not(is_last))
        def _():
            signal(barrier, {"section": me + 1})

        pl.semaphore_wait(barrier, 2 - is_first.astype(jnp.int32) - is_last.astype(jnp.int32))

    def remote(source, target, send, recv, device):
        return pltpu.make_async_remote_copy(
            src_ref=source,
            dst_ref=target,
            send_sem=send,
            recv_sem=recv,
            device_id=device,
            device_id_type=MESH,
        )

    if planes:
        beside = column + 1 - 2 * (column % 2)
        across = column + 2 - 4 * (column // 2)
        corner = 3 - column
        near = (column, beside, across, corner)
        other = {"fsdp": shard + 1 - 2 * core}
        up_rows, down_rows = features // shard_count, hidden_count // shard_count
        up_cols, down_part = hidden_count // section_count, down_rows // section_count
        share = rows // section_count

        def at_rows(start, size):
            return pl.ds(pl.multiple_of(start, size), size)

        def piece(number, full, place, which):
            if number == 0:
                return full.at[at_rows((2 * place + core) * up_rows, up_rows), at_rows(which * up_cols, up_cols)]
            return full.at[at_rows(((2 * place + core) * section_count + which) * down_part, down_part), :]

        def own_piece(number, which):
            if number == 0:
                return own_up.at[:, at_rows(which * up_cols, up_cols)]
            return own_down.at[at_rows(which * down_part, down_part), :]

        fulls = (w_up, w_down)
        holds = (hold_up, hold_down)

        def token_copy(number, m, source):
            raw, land, stage = ((patches, x_in, 0), (cotangent, g_in, stages - 1))[number]
            return remote(
                raw.at[m, at_rows(column * share, share), :],
                land.at[m, at_rows(source * share, share), :],
                token_send.at[number, m],
                token_recv.at[number, m, source],
                stage_device(stage),
            )

        def send_tokens(number, first, last):
            raw, land, stage = ((patches, x_in, 0), (cotangent, g_in, stages - 1))[number]

            @pl.when(chip != stage)
            def _():
                for m in range(first, last):
                    token_copy(number, m, chip).start()

            @pl.when(chip == stage)
            def _():
                for m in range(first, last):
                    land[m, at_rows(chip * share, share), :] = raw[m, at_rows(column * share, share), :]

        def wait_tokens(number, m):
            for source in range(chips):

                @pl.when(chip != source)
                def _():
                    token_copy(number, m, source).wait_recv()

        def scatter_copy(number, far):
            return remote(
                own_piece(number, near[far]),
                holds[number].at[column],
                scatter_send.at[number, far - 1],
                scatter_recv.at[number, column],
                {"section": near[far]},
            )

        def scatter_wait(number, source):
            hold = holds[number]
            remote(
                hold.at[source],
                hold.at[source],
                scatter_send.at[number, 0],
                scatter_recv.at[number, source],
                {"section": beside},
            ).wait_recv()

        def climb_copy(number, source, layer, place):
            return remote(
                source,
                piece(number, fulls[number], place, column),
                climb_send.at[number, layer],
                climb_recv.at[number, place],
                {"fsdp": 2 * layer + core},
            )

        def side_copy(number, way, place, which, kind, device):
            spot = piece(number, fulls[number], place, which)
            return remote(
                spot,
                spot,
                side_send.at[number, way, place],
                side_recv.at[number, kind, place],
                {"section": device},
            )

        def to_beside(number, place):
            return side_copy(number, 0, place, column, 0, beside)

        def to_across(number, place):
            return side_copy(number, 1, place, column, 1, across)

        def relay(number, place):
            if number == 0:
                return side_copy(number, 2, place, beside, 2, across)
            return side_copy(number, 2, place, across, 2, beside)

        def arrived(number, place, kind):
            side_copy(number, 0, place, near[kind + 1], kind, beside).wait_recv()

        def pair_copy(number, place, far, parity):
            which = near[far]
            full = fulls[number]
            if number == 0:
                spot = full.at[at_rows((2 * place + parity) * up_rows, up_rows), at_rows(which * up_cols, up_cols)]
            else:
                first = ((2 * place + parity) * section_count + which) * down_part
                spot = full.at[at_rows(first, down_part), :]
            return remote(
                spot, spot, pair_send.at[number, far, place], pair_recv.at[number, far, place], other
            )

        is_hub = chip == column

        def gain_copy(source, place, way, device):
            return remote(
                source,
                all_gain.at[2 * place + core],
                gain_send.at[way, place],
                gain_recv.at[2 * place + core],
                device,
            )

        def to_hub():
            return gain_copy(own_gain, chip, 0, {"fsdp": 2 * column + core})

        def from_hub(place, far):
            device = other if far == 0 else {"section": near[far]}
            return gain_copy(all_gain.at[2 * place + core], place, far + 1, device)

        def wait_gain(index):
            remote(
                all_gain.at[index], all_gain.at[index], gain_send.at[0, 0], gain_recv.at[index], other
            ).wait_recv()

        def share_gain():
            @pl.when(is_hub)
            def _():
                for place in range(chips):

                    @pl.when(place != chip)
                    def _():
                        wait_gain(2 * place + core)

                    for far in (1, 2, 3, 0):
                        from_hub(place, far).start()

            @pl.when(jnp.logical_not(is_hub))
            def _():
                for place in range(chips):
                    wait_gain(2 * place + core)
                    from_hub(place, 0).start()

        both = (0, 1)
        for number in both:
            for far in (1, 2, 3):
                scatter_copy(number, far).start()
        send_tokens(0, 0, 1)

        @pl.when(is_hub)
        def _():
            all_gain[shard] = own_gain[...]

        @pl.when(jnp.logical_not(is_hub))
        def _():
            to_hub().start()

        for far in (0, 1, 2, 3):
            layer = near[far]
            for number in both:
                if far == 0:
                    source = own_piece(number, column)
                else:
                    scatter_wait(number, layer)
                    source = holds[number].at[layer]

                @pl.when(layer != chip)
                def _():
                    climb_copy(number, source, layer, chip).start()

                @pl.when(layer == chip)
                def _():
                    spot = piece(number, fulls[number], chip, column)
                    spot[...] = source[...]

        send_tokens(0, 1, micro_count)
        send_tokens(1, 0, micro_count)

        def own_turn(step):
            place = lax.rem(chip + step, chips)
            for number in both:
                if step > 0:
                    spot = piece(number, fulls[number], place, column)
                    climb_copy(number, spot, chip, place).wait_recv()
                to_beside(number, place).start()
                to_across(number, place).start()
                pair_copy(number, place, 0, core).start()

        def side_turn(step):
            place = lax.rem(chip + step, chips)
            arrived(0, place, 0)
            relay(0, place).start()
            pair_copy(0, place, 1, core).start()
            arrived(1, place, 1)
            relay(1, place).start()
            pair_copy(1, place, 2, core).start()
            arrived(0, place, 1)
            pair_copy(0, place, 2, core).start()
            arrived(1, place, 0)
            pair_copy(1, place, 1, core).start()

        def corner_turn(step):
            place = lax.rem(chip + step, chips)
            for number in both:
                arrived(number, place, 2)
                pair_copy(number, place, 3, core).start()

        for step in range(chips + 2):
            if step < chips:
                own_turn(step)
            if 1 <= step <= chips:
                side_turn(step - 1)
            if 2 <= step:
                corner_turn(step - 2)
            if step == 1:
                share_gain()
        for place in range(chips):
            for far in (0, 1, 2, 3):
                for number in both:
                    pair_copy(number, place, far, 1 - core).wait_recv()
        for place in range(chips):
            wait_gain(2 * place + 1 - core)
        gain_blocks = jnp.sum(all_gain[...], axis=0)
        gain = jnp.concatenate(
            [gain_blocks[i : i + 1, :] for i in range(features // BLOCK)], axis=1
        )
    else:
        w_up, w_down, acc_gain = own_up, own_down, grad_gain
        gain = own_gain[:1]

    def forward_copy(m):
        return pltpu.make_async_remote_copy(
            src_ref=x_out.at[m],
            dst_ref=x_in.at[m],
            send_sem=fwd_send.at[m],
            recv_sem=fwd_recv.at[m],
            device_id=stage_device(jnp.minimum(me + 1, stages - 1)),
            device_id_type=MESH,
        )

    def backward_copy(m):
        return pltpu.make_async_remote_copy(
            src_ref=g_out.at[m],
            dst_ref=g_in.at[m],
            send_sem=bwd_send.at[m],
            recv_sem=bwd_recv.at[m],
            device_id=stage_device(jnp.maximum(me - 1, 0)),
            device_id_type=MESH,
        )

    def layer_norm(m):
        mask = embed(m)
        scale = width_inv(m)
        values = x_in[m].astype(F32) * mask
        center = jnp.sum(values, axis=-1, keepdims=True) * scale
        centered = (values - center) * mask
        variance = jnp.sum(centered * centered, axis=-1, keepdims=True) * scale
        inv_std = lax.rsqrt(variance + EPSILON)
        return centered * inv_std, inv_std

    def forward(m):
        at = pl.ds(pl.multiple_of(m * rows, rows), rows)

        @pl.when(is_first)
        def _():
            if planes:
                wait_tokens(0, m)
                x_in[m] = (x_in[m].astype(F32) * embed(m)).astype(BF16)
            else:
                x_in[m] = (patches[m].astype(F32) * embed(m)).astype(BF16)

        @pl.when(jnp.logical_not(is_first))
        def _():
            forward_copy(m).wait_recv()

        standard, _ = layer_norm(m)
        scaled = standard * gain
        normed = scaled.astype(BF16)
        for start, size in chunks(hidden_count, 512):
            part = pl.ds(start, size)
            hidden = jnp.dot(normed, w_up[:, part], preferred_element_type=F32)
            value, rise = gelu_and_slope(hidden)
            mask = hidden_mask(m, part)
            act[at, part] = (value * mask).astype(BF16)
            slope[at, part] = (rise * mask).astype(BF16)

        @pl.when(jnp.logical_not(is_last))
        def _():
            for start, size in chunks(features, 256):
                part = pl.ds(start, size)
                branch = jnp.dot(act[at, :], w_down[:, part], preferred_element_type=F32)
                out = x_in[m, :, part].astype(F32) + live(m, part) * branch
                x_out[m, :, part] = out.astype(BF16)
            forward_copy(m).start()

        return scaled

    def whole_micro(number):
        return pl.ds(pl.multiple_of(number * halves * rows, halves * rows), halves * rows)

    def forward_micro(number, carry):
        parts = [forward(number * halves + half) for half in range(halves)]
        normed_t[:, whole_micro(number)] = jnp.transpose(jnp.concatenate(parts, axis=0)).astype(BF16)
        return carry

    lax.fori_loop(0, micro_count // halves, forward_micro, 0)
    acc_gain[...] = jnp.zeros_like(acc_gain)

    def backward(m):
        at = pl.ds(pl.multiple_of(m * rows, rows), rows)

        @pl.when(is_last)
        def _():
            if planes:
                wait_tokens(1, m)
                g_in[m] = (g_in[m].astype(F32) * embed(m)).astype(BF16)
            else:
                g_in[m] = (cotangent[m].astype(F32) * embed(m)).astype(BF16)

        @pl.when(jnp.logical_not(is_last))
        def _():
            backward_copy(m).wait_recv()

        grad_float = g_in[m].astype(F32)
        branch_float = grad_float * live(m)
        branch = branch_float.astype(BF16)
        for start, size in chunks(hidden_count, 512):
            part = pl.ds(start, size)
            grad_act = contract_last(branch, w_down[part, :])
            slope[at, part] = (grad_act * slope[at, part].astype(F32)).astype(BF16)
        grad_hidden = slope[at, :]
        grad_normed = jnp.concatenate(
            [
                contract_last(grad_hidden, w_up[pl.ds(start, size), :])
                for start, size in chunks(features, 256)
            ],
            axis=1,
        )
        standard, inv_std = layer_norm(m)
        mask = embed(m)
        scale = width_inv(m)
        acc_gain[...] += jnp.sum((grad_normed * standard).reshape(-1, 8, features), axis=0)

        @pl.when(jnp.logical_not(is_first))
        def _():
            grad_standard = grad_normed * gain * mask
            first = jnp.sum(grad_standard, axis=-1, keepdims=True) * scale
            second = jnp.sum(grad_standard * standard, axis=-1, keepdims=True) * scale
            grad_x = inv_std * (grad_standard - first * mask - standard * second)
            g_out[m] = (grad_float + grad_x).astype(BF16)
            backward_copy(m).start()

        return branch_float

    def backward_micro(number, carry):
        parts = [backward(number * halves + half) for half in range(halves)]
        branch_t[:, whole_micro(number)] = jnp.transpose(jnp.concatenate(parts, axis=0)).astype(BF16)
        return carry

    lax.fori_loop(0, micro_count // halves, backward_micro, 0)

    width = 256 if hidden_count % 256 == 0 else hidden_count

    def up_grads(first, size, step):
        part = pl.ds(pl.multiple_of(step * width, width), width)
        these = pl.ds(first, size)
        return these, part, jnp.dot(normed_t[these, :], slope[:, part], preferred_element_type=F32)

    def down_grads(part):
        down = jnp.dot(branch_t[...], act[:, part], preferred_element_type=F32)
        return jnp.transpose(down).astype(BF16)

    def weight_grads(step, carry):
        these, part, up = up_grads(0, features, step)
        grad_up[these, part] = up.astype(BF16)
        grad_down[part, :] = down_grads(part)
        return carry

    def slot(full, index):
        size = full.shape[0] // shard_count
        return full.at[pl.ds(pl.multiple_of(index * size, size), size)]

    if planes:
        pairs = (pair_up, pair_down)
        firsts = (first_up, first_down)
        seconds = (second_up, second_down)
        finals = (plane_up, plane_down)
        lasts = (last_up, last_down)
        first_way = (beside, across)
        second_way = (across, beside)
        kept = (across, beside)

        def sum_pair(number, place):
            return remote(
                slot(fulls[number], 2 * place + 1 - core),
                pairs[number].at[place],
                sum_pair_send.at[number, place],
                sum_pair_recv.at[number, place],
                other,
            )

        def first_copy(number, place, index):
            which = (first_way[number], corner)[index]
            return remote(
                piece(number, fulls[number], place, which),
                firsts[number].at[place, index],
                first_send.at[number, place, index],
                first_recv.at[number, place, index],
                {"section": first_way[number]},
            )

        def second_copy(number, place):
            return remote(
                piece(number, fulls[number], place, kept[number]),
                seconds[number].at[place],
                second_send.at[number, place],
                second_recv.at[number, place],
                {"section": second_way[number]},
            )

        def plane_copy(number, place, layer):
            return remote(
                piece(number, fulls[number], place, column),
                finals[number].at[layer],
                plane_send.at[number, place],
                plane_recv.at[number, layer],
                {"fsdp": 2 * place + core},
            )

        def last_copy(number, layer, source):
            return remote(
                finals[number].at[layer],
                lasts[number].at[source],
                last_send.at[number, layer],
                last_recv.at[number, source],
                {"section": layer},
            )

        def make_grads(place):
            up_size = 2 * up_rows
            first_row = pl.multiple_of(place * up_size, up_size)

            def up_step(step, carry):
                these, part, up = up_grads(first_row, up_size, step)
                w_up[these, part] = up.astype(BF16)
                return carry

            lax.fori_loop(0, hidden_count // width, up_step, 0)
            sum_pair(0, place).start()
            down_size = 2 * down_rows
            size = math.gcd(down_size, width)

            def down_step(step, carry):
                part = at_rows(place * down_size + step * size, size)
                w_down[part, :] = down_grads(part)
                return carry

            lax.fori_loop(0, down_size // size, down_step, 0)
            sum_pair(1, place).start()

        def first_turn(place):
            for number in both:
                mine = slot(fulls[number], 2 * place + core)
                sum_pair(number, place).wait_recv()
                mine[...] = (mine[...].astype(F32) + pairs[number][place].astype(F32)).astype(BF16)
                for index in (0, 1):
                    first_copy(number, place, index).start()

        def second_turn(place):
            for number in both:
                for index in (1, 0):
                    first_copy(number, place, index).wait_recv()
                spot = piece(number, fulls[number], place, kept[number])
                total = spot[...].astype(F32) + firsts[number][place, 1].astype(F32)
                spot[...] = total.astype(BF16)
                second_copy(number, place).start()

        def plane_turn(place):
            for number in both:
                second_copy(number, place).wait_recv()
                spot = piece(number, fulls[number], place, column)
                total = spot[...].astype(F32) + firsts[number][place, 0].astype(F32)
                total = (total + seconds[number][place].astype(F32)).astype(BF16)

                @pl.when(place != chip)
                def _():
                    spot[...] = total
                    plane_copy(number, place, chip).start()

                @pl.when(place == chip)
                def _():
                    finals[number][chip] = total

        def place_at(index):
            return lax.rem(chip + chips - 1 - index + chips, chips)

        def reduce_step(index, carry):
            @pl.when(index < chips)
            def _():
                make_grads(place_at(index))
                first_turn(place_at(index))

            @pl.when(jnp.logical_and(index >= 1, index <= chips))
            def _():
                second_turn(place_at(jnp.maximum(index - 1, 0)))

            @pl.when(jnp.logical_and(index == chips, is_hub))
            def _():
                hub_turn()

            @pl.when(index >= 2)
            def _():
                plane_turn(place_at(jnp.maximum(index - 2, 0)))

            return carry

        rise = jnp.sum(acc_gain[...], axis=0, keepdims=True)
        spare = own_gain.shape[0] - features // BLOCK
        rise_rows = [rise[:, i : i + BLOCK] for i in range(0, features, BLOCK)]
        if spare:
            rise_rows.append(jnp.zeros((spare, BLOCK), F32))
        rise_own[...] = jnp.concatenate(rise_rows, axis=0)

        def rise_copy(source, target, way, device):
            return remote(source, all_rise.at[target], rise_send.at[way], rise_recv.at[target], device)

        def rise_to_hub():
            return rise_copy(rise_own, column, 0, {"section": chip})

        def rise_to_pair():
            return rise_copy(rise_own, chips, 1, other)

        def rise_to_place(place):
            return rise_copy(rise_sum, chips + 1, 2 + place, {"fsdp": 2 * place + core})

        def rise_wait(target):
            rise_copy(all_rise.at[target], target, 0, other).wait_recv()

        @pl.when(jnp.logical_not(is_hub))
        def _():
            rise_to_hub().start()

        def hub_turn():
            total = rise_own[...]
            for far in (1, 2, 3):
                rise_wait(near[far])
                total = total + all_rise[near[far]]
            rise_own[...] = total
            rise_to_pair().start()
            rise_wait(chips)
            rise_sum[...] = total + all_rise[chips]
            for place in range(chips):

                @pl.when(place != chip)
                def _():
                    rise_to_place(place).start()

        for number in both:
            for far in (1, 2, 3):
                scatter_copy(number, far).wait_send()
            for layer in range(chips):

                @pl.when(chip != layer)
                def _():
                    climb_copy(number, holds[number].at[layer], layer, chip).wait_send()

            for place in range(chips):
                to_beside(number, place).wait_send()
                to_across(number, place).wait_send()
                relay(number, place).wait_send()
                for far in (0, 1, 2, 3):
                    pair_copy(number, place, far, core).wait_send()

        @pl.when(is_hub)
        def _():
            for place in range(chips):
                for far in (0, 1, 2, 3):
                    from_hub(place, far).wait_send()

        @pl.when(jnp.logical_not(is_hub))
        def _():
            to_hub().wait_send()
            for place in range(chips):
                from_hub(place, 0).wait_send()

        lax.fori_loop(0, chips + 2, reduce_step, 0)
        for layer in reversed(range(chips)):
            for number in both:

                @pl.when(layer != chip)
                def _():
                    plane_copy(number, chip, layer).wait_recv()

                @pl.when(layer != column)
                def _():
                    last_copy(number, layer, column).start()

                @pl.when(layer == column)
                def _():
                    lasts[number][layer] = finals[number][layer]

        @pl.when(is_hub)
        def _():
            grad_gain[...] = rise_sum[...]
            rise_to_pair().wait_send()
            for place in range(chips):

                @pl.when(place != chip)
                def _():
                    rise_to_place(place).wait_send()

        @pl.when(jnp.logical_not(is_hub))
        def _():
            rise_wait(chips + 1)
            grad_gain[...] = all_rise[chips + 1]
            rise_to_hub().wait_send()

        for source in range(section_count):
            for number in both:

                @pl.when(source != column)
                def _():
                    last_copy(number, source, source).wait_recv()

            grad_up[:, pl.ds(source * up_cols, up_cols)] = last_up[source].astype(F32)
            grad_down[pl.ds(source * down_part, down_part), :] = last_down[source].astype(F32)
        for number in both:
            for place in range(chips):
                sum_pair(number, place).wait_send()
                second_copy(number, place).wait_send()
                for index in (0, 1):
                    first_copy(number, place, index).wait_send()

                @pl.when(place != chip)
                def _():
                    plane_copy(number, place, chip).wait_send()

                @pl.when(place != column)
                def _():
                    last_copy(number, place, column).wait_send()

        for number, stage in ((0, 0), (1, stages - 1)):

            @pl.when(chip != stage)
            def _():
                for m in range(micro_count):
                    token_copy(number, m, chip).wait_send()
    else:
        lax.fori_loop(0, hidden_count // width, weight_grads, 0)

    def drain(m, carry):
        @pl.when(jnp.logical_not(is_last))
        def _():
            forward_copy(m).wait_send()

        @pl.when(jnp.logical_not(is_first))
        def _():
            backward_copy(m).wait_send()

        return carry

    lax.fori_loop(0, micro_count, drain, 0)


def run_pipeline(planes, patches, cotangent, table, gain, w_up, w_down):
    section_count = lax.axis_size("section")
    shard_count = lax.axis_size("fsdp")
    micro_count, rows, features = patches.shape
    hidden_count = w_up.shape[1]
    vmem = pl.BlockSpec(memory_space=pltpu.VMEM)
    token = (micro_count, rows, features)
    tokens = micro_count * rows
    chips = shard_count // 2
    dma = pltpu.SemaphoreType.DMA
    scratch = [
        pltpu.VMEM(token, BF16),
        pltpu.VMEM(token, BF16),
        pltpu.VMEM(token, BF16),
        pltpu.VMEM(token, BF16),
        pltpu.VMEM((tokens, hidden_count), BF16),
        pltpu.VMEM((tokens, hidden_count), BF16),
        pltpu.VMEM((features, tokens), BF16),
        pltpu.VMEM((features, tokens), BF16),
        dma((micro_count,)),
        dma((micro_count,)),
        dma((micro_count,)),
        dma((micro_count,)),
    ]
    if planes:
        up_rows, down_rows = features // shard_count, hidden_count // shard_count
        up_piece = (up_rows, hidden_count // section_count)
        down_piece = (down_rows // section_count, features)
        scratch += [
            pltpu.VMEM((features, hidden_count), BF16),
            pltpu.VMEM((hidden_count, features), BF16),
            pltpu.VMEM((section_count,) + up_piece, BF16),
            pltpu.VMEM((section_count,) + down_piece, BF16),
            pltpu.VMEM((shard_count,) + gain.shape, F32),
            pltpu.VMEM((chips + 2,) + gain.shape, F32),
            pltpu.VMEM(gain.shape, F32),
            pltpu.VMEM(gain.shape, F32),
            pltpu.VMEM((8, features), F32),
            pltpu.VMEM((chips, up_rows, hidden_count), BF16),
            pltpu.VMEM((chips, down_rows, features), BF16),
            pltpu.VMEM((chips, 2) + up_piece, BF16),
            pltpu.VMEM((chips, 2) + down_piece, BF16),
            pltpu.VMEM((chips,) + up_piece, BF16),
            pltpu.VMEM((chips,) + down_piece, BF16),
            pltpu.VMEM((chips,) + up_piece, BF16),
            pltpu.VMEM((chips,) + down_piece, BF16),
            pltpu.VMEM((section_count,) + up_piece, BF16),
            pltpu.VMEM((section_count,) + down_piece, BF16),
            dma((2, micro_count)),
            dma((2, micro_count, chips)),
            dma((5, chips)),
            dma((shard_count,)),
            dma((2 + chips,)),
            dma((2 + chips,)),
            dma((2, 3)),
            dma((2, section_count)),
            dma((2, chips)),
            dma((2, chips)),
            dma((2, 3, chips)),
            dma((2, 3, chips)),
            dma((2, 4, chips)),
            dma((2, 4, chips)),
            dma((2, chips)),
            dma((2, chips)),
            dma((2, chips, 2)),
            dma((2, chips, 2)),
            dma((2, chips)),
            dma((2, chips)),
            dma((2, chips)),
            dma((2, chips)),
            dma((2, chips)),
            dma((2, section_count)),
        ]
        grads = (
            jax.ShapeDtypeStruct((up_rows, hidden_count), F32),
            jax.ShapeDtypeStruct((down_rows, features), F32),
        )
    else:
        grads = (
            jax.ShapeDtypeStruct((features, hidden_count), BF16),
            jax.ShapeDtypeStruct((hidden_count, features), BF16),
        )
    return pl.pallas_call(
        functools.partial(pipeline_kernel, section_count, shard_count),
        out_shape=grads + (jax.ShapeDtypeStruct(gain.shape, F32),),
        in_specs=[vmem] * 6,
        out_specs=(vmem, vmem, vmem),
        scratch_shapes=scratch,
        compiler_params=pltpu.CompilerParams(
            collective_id=0, has_side_effects=True, vmem_limit_bytes=VMEM_BYTES
        ),
    )(patches, cotangent, table, gain, w_up, w_down)


def per_device(patches, cotangent, embed_blocks, ratio_index, depth, w_up, w_down, ln_gain):
    section_index = lax.axis_index("section")
    shard_index = lax.axis_index("fsdp")
    shard_count = lax.axis_size("fsdp")
    micro_count, rows, features = patches.shape
    hidden_count = w_up.shape[2]
    gain_count = ln_gain.shape[1]
    section_count = lax.axis_size("section")
    down_part = w_down.shape[1] // section_count
    planes = (
        section_count == 4
        and shard_count == 2 * section_count
        and gain_count % 16 == 0
        and down_part % 16 == 0
        and hidden_count % (128 * section_count) == 0
        and rows % (16 * section_count) == 0
    )

    width = embed_blocks * BLOCK
    hidden_width = width * (6 + ratio_index) // 2
    layer = shard_index // 2 if planes else section_index
    active = (layer < depth).astype(F32)[:, None, None]
    row = lax.broadcasted_iota(jnp.int32, (micro_count, 8, hidden_count), 1)
    unit = lax.broadcasted_iota(jnp.int32, (micro_count, 8, hidden_count), 2)
    limit = jnp.where(row == 0, hidden_width[:, None, None], width[:, None, None])
    value = jnp.where(row == 2, active, 1.0)
    table = jnp.where(unit < limit, value, 0.0)
    table = jnp.where(row == 3, 1.0 / width.astype(F32)[:, None, None], table)
    start = shard_index * gain_count

    if planes:
        halves = 2 if rows % (32 * section_count) == 0 and SPLIT else 1
        gain_rows = -(-features // (8 * BLOCK)) * 8
        spot = lax.iota(jnp.int32, gain_rows * BLOCK)
        repeats = -(-gain_rows * BLOCK // gain_count)
        gain = jnp.tile(ln_gain[0].astype(F32), repeats)[: gain_rows * BLOCK]
        gain = jnp.where(spot // gain_count == shard_index, gain, 0.0).reshape(gain_rows, BLOCK)
        split = (micro_count * halves, rows // halves, features)
        own_up, own_down, gains = run_pipeline(
            True, patches.reshape(split), cotangent.reshape(split), table, gain, w_up[0], w_down[0]
        )
        own_gain = lax.dynamic_slice(gains.reshape(-1), (start,), (gain_count,))
        return (own_up[None], own_down[None], own_gain[None])

    full_up = lax.all_gather(w_up[0], "fsdp", axis=0, tiled=True)
    full_down = lax.all_gather(w_down[0], "fsdp", axis=0, tiled=True)
    gain = lax.all_gather(ln_gain[0], "fsdp", axis=0, tiled=True).astype(F32)
    gain = jnp.broadcast_to(gain[None], (8, features))
    part_up, part_down, gains = run_pipeline(
        False, patches, cotangent, table, gain, full_up, full_down
    )
    own_down = lax.psum_scatter(part_down, "fsdp", scatter_dimension=0, tiled=True)
    own_up = lax.psum_scatter(part_up, "fsdp", scatter_dimension=0, tiled=True)
    part_gain = jnp.sum(gains, axis=0)
    own_gain = lax.psum_scatter(part_gain, "fsdp", scatter_dimension=0, tiled=True)
    return (own_up.astype(F32)[None], own_down.astype(F32)[None], own_gain[None])


def solution(mesh):
    return jax.shard_map(
        per_device,
        mesh=mesh,
        in_specs=(
            P(None, "fsdp", None),
            P(None, "fsdp", None),
            P(),
            P(),
            P(),
            P("section", "fsdp", None),
            P("section", "fsdp", None),
            P("section", "fsdp"),
        ),
        out_specs=(P("section", "fsdp", None), P("section", "fsdp", None), P("section", "fsdp")),
        check_vma=False,
    )
```

```python
import functools
import math

import jax
import jax.numpy as jnp
from jax import lax
from jax.experimental import pallas as pl
from jax.experimental.pallas import tpu as pltpu
from jax.sharding import PartitionSpec as P

BLOCK = 128
SPLIT = False
LAG = 4
EPSILON = 1e-05
SCALE = 0.7978845608028654
MESH = pl.DeviceIdType.MESH
VMEM_BYTES = 66 * 1024 * 1000
BF16 = jnp.bfloat16
F32 = jnp.float32


def gelu_and_slope(hidden):
    square = hidden * hidden
    tanh = jnp.tanh(hidden * (SCALE + (SCALE * 0.044715) * square))
    half = 0.5 + 0.5 * tanh
    rise = (hidden * (0.5 * SCALE + (0.5 * SCALE * 0.134145) * square)) * (1.0 - tanh * tanh)
    return (hidden * half, half + rise)


def contract_last(left, right):
    return lax.dot_general(left, right, (((1,), (1,)), ((), ())), preferred_element_type=F32)


def chunks(total, size):
    size = size if total % size == 0 else total
    return [(start, size) for start in range(0, total, size)]


def signal(semaphore, device):
    pl.semaphore_signal(semaphore, inc=1, device_id=device, device_id_type=MESH)


def pipeline_kernel(
    section_count,
    shard_count,
    patches,
    cotangent,
    table,
    own_gain,
    own_up,
    own_down,
    grad_up,
    grad_down,
    grad_gain,
    x_in,
    x_out,
    g_in,
    g_out,
    act,
    slope,
    normed_t,
    branch_t,
    fwd_send,
    fwd_recv,
    bwd_send,
    bwd_recv,
    w_up=None,
    w_down=None,
    hold_up=None,
    hold_down=None,
    all_gain=None,
    all_rise=None,
    rise_own=None,
    rise_sum=None,
    acc_gain=None,
    pair_up=None,
    pair_down=None,
    first_up=None,
    first_down=None,
    second_up=None,
    second_down=None,
    plane_up=None,
    plane_down=None,
    last_up=None,
    last_down=None,
    token_send=None,
    token_recv=None,
    gain_send=None,
    gain_recv=None,
    rise_send=None,
    rise_recv=None,
    scatter_send=None,
    scatter_recv=None,
    climb_send=None,
    climb_recv=None,
    side_send=None,
    side_recv=None,
    pair_send=None,
    pair_recv=None,
    sum_pair_send=None,
    sum_pair_recv=None,
    first_send=None,
    first_recv=None,
    second_send=None,
    second_recv=None,
    plane_send=None,
    plane_recv=None,
    last_send=None,
    last_recv=None,
):
    planes = w_up is not None
    column = lax.axis_index("section")
    shard = lax.axis_index("fsdp")
    chip = shard // 2
    core = shard % 2
    chips = shard_count // 2
    me = chip if planes else column
    stages = chips if planes else section_count
    is_first = me == 0
    is_last = me == stages - 1
    micro_count, rows, features = patches.shape
    hidden_count = table.shape[2]
    features_all = pl.ds(0, features)
    halves = micro_count // table.shape[0]

    def hidden_mask(m, part):
        return table[m // halves, 0:1, part]

    def embed(m, part=features_all):
        return table[m // halves, 1:2, part]

    def live(m, part=features_all):
        return table[m // halves, 2:3, part]

    def width_inv(m):
        return table[m // halves, 3:4, 0:1]

    def stage_device(stage):
        return {"fsdp": 2 * stage + core} if planes else {"section": stage}

    barrier = pltpu.get_barrier_semaphore()
    if planes:
        for step in range(1, section_count):
            signal(barrier, {"section": lax.rem(column + step, section_count)})
            signal(barrier, {"fsdp": lax.rem(shard + 2 * step, shard_count)})
        signal(barrier, {"fsdp": shard + 1 - 2 * core})
        pl.semaphore_wait(barrier, 2 * section_count - 1)
    else:

        @pl.when(jnp.logical_not(is_first))
        def _():
            signal(barrier, {"section": me - 1})

        @pl.when(jnp.logical_not(is_last))
        def _():
            signal(barrier, {"section": me + 1})

        pl.semaphore_wait(barrier, 2 - is_first.astype(jnp.int32) - is_last.astype(jnp.int32))

    def remote(source, target, send, recv, device):
        return pltpu.make_async_remote_copy(
            src_ref=source,
            dst_ref=target,
            send_sem=send,
            recv_sem=recv,
            device_id=device,
            device_id_type=MESH,
        )

    if planes:
        beside = column + 1 - 2 * (column % 2)
        across = column + 2 - 4 * (column // 2)
        corner = 3 - column
        near = (column, beside, across, corner)
        other = {"fsdp": shard + 1 - 2 * core}
        up_rows, down_rows = features // shard_count, hidden_count // shard_count
        up_cols, down_part = hidden_count // section_count, down_rows // section_count
        share = rows // section_count

        def at_rows(start, size):
            return pl.ds(pl.multiple_of(start, size), size)

        def piece(number, full, place, which):
            if number == 0:
                return full.at[at_rows((2 * place + core) * up_rows, up_rows), at_rows(which * up_cols, up_cols)]
            return full.at[at_rows(((2 * place + core) * section_count + which) * down_part, down_part), :]

        def own_piece(number, which):
            if number == 0:
                return own_up.at[:, at_rows(which * up_cols, up_cols)]
            return own_down.at[at_rows(which * down_part, down_part), :]

        fulls = (w_up, w_down)
        holds = (hold_up, hold_down)

        def token_copy(number, m, source):
            raw, land, stage = ((patches, x_in, 0), (cotangent, g_in, stages - 1))[number]
            return remote(
                raw.at[m, at_rows(column * share, share), :],
                land.at[m, at_rows(source * share, share), :],
                token_send.at[number, m],
                token_recv.at[number, m, source],
                stage_device(stage),
            )

        def send_tokens(number, first, last):
            raw, land, stage = ((patches, x_in, 0), (cotangent, g_in, stages - 1))[number]

            @pl.when(chip != stage)
            def _():
                for m in range(first, last):
                    token_copy(number, m, chip).start()

            @pl.when(chip == stage)
            def _():
                for m in range(first, last):
                    land[m, at_rows(chip * share, share), :] = raw[m, at_rows(column * share, share), :]

        def wait_tokens(number, m):
            for source in range(chips):

                @pl.when(chip != source)
                def _():
                    token_copy(number, m, source).wait_recv()

        def scatter_copy(number, far):
            return remote(
                own_piece(number, near[far]),
                holds[number].at[column],
                scatter_send.at[number, far - 1],
                scatter_recv.at[number, column],
                {"section": near[far]},
            )

        def scatter_wait(number, source):
            hold = holds[number]
            remote(
                hold.at[source],
                hold.at[source],
                scatter_send.at[number, 0],
                scatter_recv.at[number, source],
                {"section": beside},
            ).wait_recv()

        def climb_copy(number, source, layer, place):
            return remote(
                source,
                piece(number, fulls[number], place, column),
                climb_send.at[number, layer],
                climb_recv.at[number, place],
                {"fsdp": 2 * layer + core},
            )

        def side_copy(number, way, place, which, kind, device):
            spot = piece(number, fulls[number], place, which)
            return remote(
                spot,
                spot,
                side_send.at[number, way, place],
                side_recv.at[number, kind, place],
                {"section": device},
            )

        def to_beside(number, place):
            return side_copy(number, 0, place, column, 0, beside)

        def to_across(number, place):
            return side_copy(number, 1, place, column, 1, across)

        def relay(number, place):
            if number == 0:
                return side_copy(number, 2, place, beside, 2, across)
            return side_copy(number, 2, place, across, 2, beside)

        def arrived(number, place, kind):
            side_copy(number, 0, place, near[kind + 1], kind, beside).wait_recv()

        def pair_copy(number, place, far, parity):
            which = near[far]
            full = fulls[number]
            if number == 0:
                spot = full.at[at_rows((2 * place + parity) * up_rows, up_rows), at_rows(which * up_cols, up_cols)]
            else:
                first = ((2 * place + parity) * section_count + which) * down_part
                spot = full.at[at_rows(first, down_part), :]
            return remote(
                spot, spot, pair_send.at[number, far, place], pair_recv.at[number, far, place], other
            )

        is_hub = chip == column

        def gain_copy(source, place, way, device):
            return remote(
                source,
                all_gain.at[2 * place + core],
                gain_send.at[way, place],
                gain_recv.at[2 * place + core],
                device,
            )

        def to_hub():
            return gain_copy(own_gain, chip, 0, {"fsdp": 2 * column + core})

        def from_hub(place, far):
            device = other if far == 0 else {"section": near[far]}
            return gain_copy(all_gain.at[2 * place + core], place, far + 1, device)

        def wait_gain(index):
            remote(
                all_gain.at[index], all_gain.at[index], gain_send.at[0, 0], gain_recv.at[index], other
            ).wait_recv()

        def share_gain():
            @pl.when(is_hub)
            def _():
                for place in range(chips):

                    @pl.when(place != chip)
                    def _():
                        wait_gain(2 * place + core)

                    for far in (1, 2, 3, 0):
                        from_hub(place, far).start()

            @pl.when(jnp.logical_not(is_hub))
            def _():
                for place in range(chips):
                    wait_gain(2 * place + core)
                    from_hub(place, 0).start()

        both = (0, 1)
        for number in both:
            for far in (1, 2, 3):
                scatter_copy(number, far).start()
        send_tokens(0, 0, 1)

        @pl.when(is_hub)
        def _():
            all_gain[shard] = own_gain[...]

        @pl.when(jnp.logical_not(is_hub))
        def _():
            to_hub().start()

        for far in (0, 1, 2, 3):
            layer = near[far]
            for number in both:
                if far == 0:
                    source = own_piece(number, column)
                else:
                    scatter_wait(number, layer)
                    source = holds[number].at[layer]

                @pl.when(layer != chip)
                def _():
                    climb_copy(number, source, layer, chip).start()

                @pl.when(layer == chip)
                def _():
                    spot = piece(number, fulls[number], chip, column)
                    spot[...] = source[...]

        def own_turn(step):
            place = lax.rem(chip + step, chips)
            for number in both:
                if step > 0:
                    spot = piece(number, fulls[number], place, column)
                    climb_copy(number, spot, chip, place).wait_recv()
                to_beside(number, place).start()
                to_across(number, place).start()
                pair_copy(number, place, 0, core).start()

        def side_turn(step):
            place = lax.rem(chip + step, chips)
            arrived(0, place, 0)
            relay(0, place).start()
            pair_copy(0, place, 1, core).start()
            arrived(1, place, 1)
            relay(1, place).start()
            pair_copy(1, place, 2, core).start()
            arrived(0, place, 1)
            pair_copy(0, place, 2, core).start()
            arrived(1, place, 0)
            pair_copy(1, place, 1, core).start()

        def corner_turn(step):
            place = lax.rem(chip + step, chips)
            for number in both:
                arrived(number, place, 2)
                pair_copy(number, place, 3, core).start()

        for step in range(chips + 2):
            if step < chips:
                own_turn(step)
            if step == chips - 1:
                send_tokens(0, 1, micro_count)
                send_tokens(1, 0, micro_count)
            if 1 <= step <= chips:
                side_turn(step - 1)
            if 2 <= step:
                corner_turn(step - 2)
            if step == 1:
                share_gain()
        for place in range(chips):
            for far in (0, 1, 2, 3):
                for number in both:
                    pair_copy(number, place, far, 1 - core).wait_recv()
        for place in range(chips):
            wait_gain(2 * place + 1 - core)
        gain_blocks = jnp.sum(all_gain[...], axis=0)
        gain = jnp.concatenate(
            [gain_blocks[i : i + 1, :] for i in range(features // BLOCK)], axis=1
        )
    else:
        w_up, w_down, acc_gain = own_up, own_down, grad_gain
        gain = own_gain[:1]

    def forward_copy(m):
        return pltpu.make_async_remote_copy(
            src_ref=x_out.at[m],
            dst_ref=x_in.at[m],
            send_sem=fwd_send.at[m],
            recv_sem=fwd_recv.at[m],
            device_id=stage_device(jnp.minimum(me + 1, stages - 1)),
            device_id_type=MESH,
        )

    def backward_copy(m):
        return pltpu.make_async_remote_copy(
            src_ref=g_out.at[m],
            dst_ref=g_in.at[m],
            send_sem=bwd_send.at[m],
            recv_sem=bwd_recv.at[m],
            device_id=stage_device(jnp.maximum(me - 1, 0)),
            device_id_type=MESH,
        )

    def layer_norm(m):
        mask = embed(m)
        scale = width_inv(m)
        values = x_in[m].astype(F32) * mask
        center = jnp.sum(values, axis=-1, keepdims=True) * scale
        centered = (values - center) * mask
        variance = jnp.sum(centered * centered, axis=-1, keepdims=True) * scale
        inv_std = lax.rsqrt(variance + EPSILON)
        return centered * inv_std, inv_std

    def forward(m):
        at = pl.ds(pl.multiple_of(m * rows, rows), rows)

        @pl.when(is_first)
        def _():
            if planes:
                wait_tokens(0, m)
                x_in[m] = (x_in[m].astype(F32) * embed(m)).astype(BF16)
            else:
                x_in[m] = (patches[m].astype(F32) * embed(m)).astype(BF16)

        @pl.when(jnp.logical_not(is_first))
        def _():
            forward_copy(m).wait_recv()

        standard, _ = layer_norm(m)
        scaled = standard * gain
        normed = scaled.astype(BF16)
        for start, size in chunks(hidden_count, 512):
            part = pl.ds(start, size)
            hidden = jnp.dot(normed, w_up[:, part], preferred_element_type=F32)
            value, rise = gelu_and_slope(hidden)
            mask = hidden_mask(m, part)
            act[at, part] = (value * mask).astype(BF16)
            slope[at, part] = (rise * mask).astype(BF16)

        @pl.when(jnp.logical_not(is_last))
        def _():
            for start, size in chunks(features, 256):
                part = pl.ds(start, size)
                branch = jnp.dot(act[at, :], w_down[:, part], preferred_element_type=F32)
                out = x_in[m, :, part].astype(F32) + live(m, part) * branch
                x_out[m, :, part] = out.astype(BF16)
            forward_copy(m).start()

        return scaled

    def whole_micro(number):
        return pl.ds(pl.multiple_of(number * halves * rows, halves * rows), halves * rows)

    def forward_micro(number, carry):
        parts = [forward(number * halves + half) for half in range(halves)]
        normed_t[:, whole_micro(number)] = jnp.transpose(jnp.concatenate(parts, axis=0)).astype(BF16)
        return carry

    acc_gain[...] = jnp.zeros_like(acc_gain)

    def backward(m):
        at = pl.ds(pl.multiple_of(m * rows, rows), rows)

        @pl.when(is_last)
        def _():
            if planes:
                wait_tokens(1, m)
                g_in[m] = (g_in[m].astype(F32) * embed(m)).astype(BF16)
            else:
                g_in[m] = (cotangent[m].astype(F32) * embed(m)).astype(BF16)

        @pl.when(jnp.logical_not(is_last))
        def _():
            backward_copy(m).wait_recv()

        grad_float = g_in[m].astype(F32)
        branch_float = grad_float * live(m)
        branch = branch_float.astype(BF16)
        for start, size in chunks(hidden_count, 512):
            part = pl.ds(start, size)
            grad_act = contract_last(branch, w_down[part, :])
            slope[at, part] = (grad_act * slope[at, part].astype(F32)).astype(BF16)
        grad_hidden = slope[at, :]
        grad_normed = jnp.concatenate(
            [
                contract_last(grad_hidden, w_up[pl.ds(start, size), :])
                for start, size in chunks(features, 256)
            ],
            axis=1,
        )
        standard, inv_std = layer_norm(m)
        mask = embed(m)
        scale = width_inv(m)
        acc_gain[...] += jnp.sum((grad_normed * standard).reshape(-1, 8, features), axis=0)

        @pl.when(jnp.logical_not(is_first))
        def _():
            grad_standard = grad_normed * gain * mask
            first = jnp.sum(grad_standard, axis=-1, keepdims=True) * scale
            second = jnp.sum(grad_standard * standard, axis=-1, keepdims=True) * scale
            grad_x = inv_std * (grad_standard - first * mask - standard * second)
            g_out[m] = (grad_float + grad_x).astype(BF16)
            backward_copy(m).start()

        return branch_float

    def backward_micro(number, carry):
        parts = [backward(number * halves + half) for half in range(halves)]
        branch_t[:, whole_micro(number)] = jnp.transpose(jnp.concatenate(parts, axis=0)).astype(BF16)
        return carry

    micro_total = micro_count // halves
    lag = jnp.minimum(LAG * (stages - 1 - me), micro_total)

    def turn(number, carry):
        @pl.when(number < micro_total)
        def _():
            forward_micro(jnp.minimum(number, micro_total - 1), 0)

        late = number - lag

        @pl.when(jnp.logical_and(late >= 0, late < micro_total))
        def _():
            backward_micro(jnp.clip(late, 0, micro_total - 1), 0)

        return carry

    lax.fori_loop(0, 2 * micro_total, turn, 0)

    width = 256 if hidden_count % 256 == 0 else hidden_count

    def up_grads(first, size, step):
        part = pl.ds(pl.multiple_of(step * width, width), width)
        these = pl.ds(first, size)
        return these, part, jnp.dot(normed_t[these, :], slope[:, part], preferred_element_type=F32)

    def down_grads(part):
        down = jnp.dot(branch_t[...], act[:, part], preferred_element_type=F32)
        return jnp.transpose(down).astype(BF16)

    def weight_grads(step, carry):
        these, part, up = up_grads(0, features, step)
        grad_up[these, part] = up.astype(BF16)
        grad_down[part, :] = down_grads(part)
        return carry

    def slot(full, index):
        size = full.shape[0] // shard_count
        return full.at[pl.ds(pl.multiple_of(index * size, size), size)]

    if planes:
        pairs = (pair_up, pair_down)
        firsts = (first_up, first_down)
        seconds = (second_up, second_down)
        finals = (plane_up, plane_down)
        lasts = (last_up, last_down)
        first_way = (beside, across)
        second_way = (across, beside)
        kept = (across, beside)

        def sum_pair(number, place):
            return remote(
                slot(fulls[number], 2 * place + 1 - core),
                pairs[number].at[place],
                sum_pair_send.at[number, place],
                sum_pair_recv.at[number, place],
                other,
            )

        def first_copy(number, place, index):
            which = (first_way[number], corner)[index]
            return remote(
                piece(number, fulls[number], place, which),
                firsts[number].at[place, index],
                first_send.at[number, place, index],
                first_recv.at[number, place, index],
                {"section": first_way[number]},
            )

        def second_copy(number, place):
            return remote(
                piece(number, fulls[number], place, kept[number]),
                seconds[number].at[place],
                second_send.at[number, place],
                second_recv.at[number, place],
                {"section": second_way[number]},
            )

        def plane_copy(number, place, layer):
            return remote(
                piece(number, fulls[number], place, column),
                finals[number].at[layer],
                plane_send.at[number, place],
                plane_recv.at[number, layer],
                {"fsdp": 2 * place + core},
            )

        def last_copy(number, layer, source):
            return remote(
                finals[number].at[layer],
                lasts[number].at[source],
                last_send.at[number, layer],
                last_recv.at[number, source],
                {"section": layer},
            )

        def make_grads(place):
            up_size = 2 * up_rows
            first_row = pl.multiple_of(place * up_size, up_size)

            def up_step(step, carry):
                these, part, up = up_grads(first_row, up_size, step)
                w_up[these, part] = up.astype(BF16)
                return carry

            lax.fori_loop(0, hidden_count // width, up_step, 0)
            sum_pair(0, place).start()
            down_size = 2 * down_rows
            size = math.gcd(down_size, width)

            def down_step(step, carry):
                part = at_rows(place * down_size + step * size, size)
                w_down[part, :] = down_grads(part)
                return carry

            lax.fori_loop(0, down_size // size, down_step, 0)
            sum_pair(1, place).start()

        def first_turn(place):
            for number in both:
                mine = slot(fulls[number], 2 * place + core)
                sum_pair(number, place).wait_recv()
                mine[...] = (mine[...].astype(F32) + pairs[number][place].astype(F32)).astype(BF16)
                for index in (0, 1):
                    first_copy(number, place, index).start()

        def second_turn(place):
            for number in both:
                for index in (1, 0):
                    first_copy(number, place, index).wait_recv()
                spot = piece(number, fulls[number], place, kept[number])
                total = spot[...].astype(F32) + firsts[number][place, 1].astype(F32)
                spot[...] = total.astype(BF16)
                second_copy(number, place).start()

        def plane_turn(place):
            for number in both:
                second_copy(number, place).wait_recv()
                spot = piece(number, fulls[number], place, column)
                total = spot[...].astype(F32) + firsts[number][place, 0].astype(F32)
                total = (total + seconds[number][place].astype(F32)).astype(BF16)

                @pl.when(place != chip)
                def _():
                    spot[...] = total
                    plane_copy(number, place, chip).start()

                @pl.when(place == chip)
                def _():
                    finals[number][chip] = total

        def place_at(index):
            return lax.rem(chip + chips - 1 - index + chips, chips)

        def reduce_step(index, carry):
            @pl.when(index < chips)
            def _():
                make_grads(place_at(index))
                first_turn(place_at(index))

            @pl.when(jnp.logical_and(index >= 1, index <= chips))
            def _():
                second_turn(place_at(jnp.maximum(index - 1, 0)))

            @pl.when(jnp.logical_and(index == chips, is_hub))
            def _():
                hub_turn()

            @pl.when(index >= 2)
            def _():
                plane_turn(place_at(jnp.maximum(index - 2, 0)))

            return carry

        rise = jnp.sum(acc_gain[...], axis=0, keepdims=True)
        spare = own_gain.shape[0] - features // BLOCK
        rise_rows = [rise[:, i : i + BLOCK] for i in range(0, features, BLOCK)]
        if spare:
            rise_rows.append(jnp.zeros((spare, BLOCK), F32))
        rise_own[...] = jnp.concatenate(rise_rows, axis=0)

        def rise_copy(source, target, way, device):
            return remote(source, all_rise.at[target], rise_send.at[way], rise_recv.at[target], device)

        def rise_to_hub():
            return rise_copy(rise_own, column, 0, {"section": chip})

        def rise_to_pair():
            return rise_copy(rise_own, chips, 1, other)

        def rise_to_place(place):
            return rise_copy(rise_sum, chips + 1, 2 + place, {"fsdp": 2 * place + core})

        def rise_wait(target):
            rise_copy(all_rise.at[target], target, 0, other).wait_recv()

        @pl.when(jnp.logical_not(is_hub))
        def _():
            rise_to_hub().start()

        def hub_turn():
            total = rise_own[...]
            for far in (1, 2, 3):
                rise_wait(near[far])
                total = total + all_rise[near[far]]
            rise_own[...] = total
            rise_to_pair().start()
            rise_wait(chips)
            rise_sum[...] = total + all_rise[chips]
            for place in range(chips):

                @pl.when(place != chip)
                def _():
                    rise_to_place(place).start()

        for number in both:
            for far in (1, 2, 3):
                scatter_copy(number, far).wait_send()
            for layer in range(chips):

                @pl.when(chip != layer)
                def _():
                    climb_copy(number, holds[number].at[layer], layer, chip).wait_send()

            for place in range(chips):
                to_beside(number, place).wait_send()
                to_across(number, place).wait_send()
                relay(number, place).wait_send()
                for far in (0, 1, 2, 3):
                    pair_copy(number, place, far, core).wait_send()

        @pl.when(is_hub)
        def _():
            for place in range(chips):
                for far in (0, 1, 2, 3):
                    from_hub(place, far).wait_send()

        @pl.when(jnp.logical_not(is_hub))
        def _():
            to_hub().wait_send()
            for place in range(chips):
                from_hub(place, 0).wait_send()

        lax.fori_loop(0, chips + 2, reduce_step, 0)
        for layer in reversed(range(chips)):
            for number in both:

                @pl.when(layer != chip)
                def _():
                    plane_copy(number, chip, layer).wait_recv()

                @pl.when(layer != column)
                def _():
                    last_copy(number, layer, column).start()

                @pl.when(layer == column)
                def _():
                    lasts[number][layer] = finals[number][layer]

        @pl.when(is_hub)
        def _():
            grad_gain[...] = rise_sum[...]
            rise_to_pair().wait_send()
            for place in range(chips):

                @pl.when(place != chip)
                def _():
                    rise_to_place(place).wait_send()

        @pl.when(jnp.logical_not(is_hub))
        def _():
            rise_wait(chips + 1)
            grad_gain[...] = all_rise[chips + 1]
            rise_to_hub().wait_send()

        for source in range(section_count):
            for number in both:

                @pl.when(source != column)
                def _():
                    last_copy(number, source, source).wait_recv()

            grad_up[:, pl.ds(source * up_cols, up_cols)] = last_up[source].astype(F32)
            grad_down[pl.ds(source * down_part, down_part), :] = last_down[source].astype(F32)
        for number in both:
            for place in range(chips):
                sum_pair(number, place).wait_send()
                second_copy(number, place).wait_send()
                for index in (0, 1):
                    first_copy(number, place, index).wait_send()

                @pl.when(place != chip)
                def _():
                    plane_copy(number, place, chip).wait_send()

                @pl.when(place != column)
                def _():
                    last_copy(number, place, column).wait_send()

        for number, stage in ((0, 0), (1, stages - 1)):

            @pl.when(chip != stage)
            def _():
                for m in range(micro_count):
                    token_copy(number, m, chip).wait_send()
    else:
        lax.fori_loop(0, hidden_count // width, weight_grads, 0)

    def drain(m, carry):
        @pl.when(jnp.logical_not(is_last))
        def _():
            forward_copy(m).wait_send()

        @pl.when(jnp.logical_not(is_first))
        def _():
            backward_copy(m).wait_send()

        return carry

    lax.fori_loop(0, micro_count, drain, 0)


def run_pipeline(planes, patches, cotangent, table, gain, w_up, w_down):
    section_count = lax.axis_size("section")
    shard_count = lax.axis_size("fsdp")
    micro_count, rows, features = patches.shape
    hidden_count = w_up.shape[1]
    vmem = pl.BlockSpec(memory_space=pltpu.VMEM)
    token = (micro_count, rows, features)
    tokens = micro_count * rows
    chips = shard_count // 2
    dma = pltpu.SemaphoreType.DMA
    scratch = [
        pltpu.VMEM(token, BF16),
        pltpu.VMEM(token, BF16),
        pltpu.VMEM(token, BF16),
        pltpu.VMEM(token, BF16),
        pltpu.VMEM((tokens, hidden_count), BF16),
        pltpu.VMEM((tokens, hidden_count), BF16),
        pltpu.VMEM((features, tokens), BF16),
        pltpu.VMEM((features, tokens), BF16),
        dma((micro_count,)),
        dma((micro_count,)),
        dma((micro_count,)),
        dma((micro_count,)),
    ]
    if planes:
        up_rows, down_rows = features // shard_count, hidden_count // shard_count
        up_piece = (up_rows, hidden_count // section_count)
        down_piece = (down_rows // section_count, features)
        scratch += [
            pltpu.VMEM((features, hidden_count), BF16),
            pltpu.VMEM((hidden_count, features), BF16),
            pltpu.VMEM((section_count,) + up_piece, BF16),
            pltpu.VMEM((section_count,) + down_piece, BF16),
            pltpu.VMEM((shard_count,) + gain.shape, F32),
            pltpu.VMEM((chips + 2,) + gain.shape, F32),
            pltpu.VMEM(gain.shape, F32),
            pltpu.VMEM(gain.shape, F32),
            pltpu.VMEM((8, features), F32),
            pltpu.VMEM((chips, up_rows, hidden_count), BF16),
            pltpu.VMEM((chips, down_rows, features), BF16),
            pltpu.VMEM((chips, 2) + up_piece, BF16),
            pltpu.VMEM((chips, 2) + down_piece, BF16),
            pltpu.VMEM((chips,) + up_piece, BF16),
            pltpu.VMEM((chips,) + down_piece, BF16),
            pltpu.VMEM((chips,) + up_piece, BF16),
            pltpu.VMEM((chips,) + down_piece, BF16),
            pltpu.VMEM((section_count,) + up_piece, BF16),
            pltpu.VMEM((section_count,) + down_piece, BF16),
            dma((2, micro_count)),
            dma((2, micro_count, chips)),
            dma((5, chips)),
            dma((shard_count,)),
            dma((2 + chips,)),
            dma((2 + chips,)),
            dma((2, 3)),
            dma((2, section_count)),
            dma((2, chips)),
            dma((2, chips)),
            dma((2, 3, chips)),
            dma((2, 3, chips)),
            dma((2, 4, chips)),
            dma((2, 4, chips)),
            dma((2, chips)),
            dma((2, chips)),
            dma((2, chips, 2)),
            dma((2, chips, 2)),
            dma((2, chips)),
            dma((2, chips)),
            dma((2, chips)),
            dma((2, chips)),
            dma((2, chips)),
            dma((2, section_count)),
        ]
        grads = (
            jax.ShapeDtypeStruct((up_rows, hidden_count), F32),
            jax.ShapeDtypeStruct((down_rows, features), F32),
        )
    else:
        grads = (
            jax.ShapeDtypeStruct((features, hidden_count), BF16),
            jax.ShapeDtypeStruct((hidden_count, features), BF16),
        )
    return pl.pallas_call(
        functools.partial(pipeline_kernel, section_count, shard_count),
        out_shape=grads + (jax.ShapeDtypeStruct(gain.shape, F32),),
        in_specs=[vmem] * 6,
        out_specs=(vmem, vmem, vmem),
        scratch_shapes=scratch,
        compiler_params=pltpu.CompilerParams(
            collective_id=0, has_side_effects=True, vmem_limit_bytes=VMEM_BYTES
        ),
    )(patches, cotangent, table, gain, w_up, w_down)


def per_device(patches, cotangent, embed_blocks, ratio_index, depth, w_up, w_down, ln_gain):
    section_index = lax.axis_index("section")
    shard_index = lax.axis_index("fsdp")
    shard_count = lax.axis_size("fsdp")
    micro_count, rows, features = patches.shape
    hidden_count = w_up.shape[2]
    gain_count = ln_gain.shape[1]
    section_count = lax.axis_size("section")
    down_part = w_down.shape[1] // section_count
    planes = (
        section_count == 4
        and shard_count == 2 * section_count
        and gain_count % 16 == 0
        and down_part % 16 == 0
        and hidden_count % (128 * section_count) == 0
        and rows % (16 * section_count) == 0
    )

    width = embed_blocks * BLOCK
    hidden_width = width * (6 + ratio_index) // 2
    layer = shard_index // 2 if planes else section_index
    active = (layer < depth).astype(F32)[:, None, None]
    row = lax.broadcasted_iota(jnp.int32, (micro_count, 8, hidden_count), 1)
    unit = lax.broadcasted_iota(jnp.int32, (micro_count, 8, hidden_count), 2)
    limit = jnp.where(row == 0, hidden_width[:, None, None], width[:, None, None])
    value = jnp.where(row == 2, active, 1.0)
    table = jnp.where(unit < limit, value, 0.0)
    table = jnp.where(row == 3, 1.0 / width.astype(F32)[:, None, None], table)
    start = shard_index * gain_count

    if planes:
        halves = 2 if rows % (32 * section_count) == 0 and SPLIT else 1
        gain_rows = -(-features // (8 * BLOCK)) * 8
        spot = lax.iota(jnp.int32, gain_rows * BLOCK)
        repeats = -(-gain_rows * BLOCK // gain_count)
        gain = jnp.tile(ln_gain[0].astype(F32), repeats)[: gain_rows * BLOCK]
        gain = jnp.where(spot // gain_count == shard_index, gain, 0.0).reshape(gain_rows, BLOCK)
        split = (micro_count * halves, rows // halves, features)
        own_up, own_down, gains = run_pipeline(
            True, patches.reshape(split), cotangent.reshape(split), table, gain, w_up[0], w_down[0]
        )
        own_gain = lax.dynamic_slice(gains.reshape(-1), (start,), (gain_count,))
        return (own_up[None], own_down[None], own_gain[None])

    full_up = lax.all_gather(w_up[0], "fsdp", axis=0, tiled=True)
    full_down = lax.all_gather(w_down[0], "fsdp", axis=0, tiled=True)
    gain = lax.all_gather(ln_gain[0], "fsdp", axis=0, tiled=True).astype(F32)
    gain = jnp.broadcast_to(gain[None], (8, features))
    part_up, part_down, gains = run_pipeline(
        False, patches, cotangent, table, gain, full_up, full_down
    )
    own_down = lax.psum_scatter(part_down, "fsdp", scatter_dimension=0, tiled=True)
    own_up = lax.psum_scatter(part_up, "fsdp", scatter_dimension=0, tiled=True)
    part_gain = jnp.sum(gains, axis=0)
    own_gain = lax.psum_scatter(part_gain, "fsdp", scatter_dimension=0, tiled=True)
    return (own_up.astype(F32)[None], own_down.astype(F32)[None], own_gain[None])


def solution(mesh):
    return jax.shard_map(
        per_device,
        mesh=mesh,
        in_specs=(
            P(None, "fsdp", None),
            P(None, "fsdp", None),
            P(),
            P(),
            P(),
            P("section", "fsdp", None),
            P("section", "fsdp", None),
            P("section", "fsdp"),
        ),
        out_specs=(P("section", "fsdp", None), P("section", "fsdp", None), P("section", "fsdp")),
        check_vma=False,
    )
```

```python
import functools
import math

import jax
import jax.numpy as jnp
from jax import lax
from jax.experimental import pallas as pl
from jax.experimental.pallas import tpu as pltpu
from jax.sharding import PartitionSpec as P

BLOCK = 128
SPLIT = False
LAG = 4
EPSILON = 1e-05
SCALE = 0.7978845608028654
MESH = pl.DeviceIdType.MESH
VMEM_BYTES = 66 * 1024 * 1000
BF16 = jnp.bfloat16
F32 = jnp.float32


def gelu_and_slope(hidden):
    square = hidden * hidden
    tanh = jnp.tanh(hidden * (SCALE + (SCALE * 0.044715) * square))
    half = 0.5 + 0.5 * tanh
    rise = (hidden * (0.5 * SCALE + (0.5 * SCALE * 0.134145) * square)) * (1.0 - tanh * tanh)
    return (hidden * half, half + rise)


def contract_last(left, right):
    return lax.dot_general(left, right, (((1,), (1,)), ((), ())), preferred_element_type=F32)


def chunks(total, size):
    size = size if total % size == 0 else total
    return [(start, size) for start in range(0, total, size)]


def signal(semaphore, device):
    pl.semaphore_signal(semaphore, inc=1, device_id=device, device_id_type=MESH)


def pipeline_kernel(
    section_count,
    shard_count,
    patches,
    cotangent,
    embed_blocks,
    ratio_index,
    depth,
    own_gain,
    own_up,
    own_down,
    grad_up,
    grad_down,
    grad_gain,
    x_in,
    x_out,
    g_in,
    g_out,
    act,
    slope,
    normed_t,
    branch_t,
    table,
    fwd_send,
    fwd_recv,
    bwd_send,
    bwd_recv,
    w_up=None,
    w_down=None,
    hold_up=None,
    hold_down=None,
    all_gain=None,
    all_rise=None,
    rise_own=None,
    rise_sum=None,
    acc_gain=None,
    pair_up=None,
    pair_down=None,
    first_up=None,
    first_down=None,
    second_up=None,
    second_down=None,
    plane_up=None,
    plane_down=None,
    last_up=None,
    last_down=None,
    token_send=None,
    token_recv=None,
    gain_send=None,
    gain_recv=None,
    rise_send=None,
    rise_recv=None,
    scatter_send=None,
    scatter_recv=None,
    climb_send=None,
    climb_recv=None,
    side_send=None,
    side_recv=None,
    pair_send=None,
    pair_recv=None,
    sum_pair_send=None,
    sum_pair_recv=None,
    first_send=None,
    first_recv=None,
    second_send=None,
    second_recv=None,
    plane_send=None,
    plane_recv=None,
    last_send=None,
    last_recv=None,
):
    planes = w_up is not None
    column = lax.axis_index("section")
    shard = lax.axis_index("fsdp")
    chip = shard // 2
    core = shard % 2
    chips = shard_count // 2
    me = chip if planes else column
    stages = chips if planes else section_count
    is_first = me == 0
    is_last = me == stages - 1
    micro_count, rows, features = patches.shape
    hidden_count = own_up.shape[1]
    features_all = pl.ds(0, features)
    halves = micro_count // table.shape[0]

    def build_table():
        for m in range(table.shape[0]):
            unit = lax.broadcasted_iota(jnp.int32, (1, hidden_count), 1)
            blocks = embed_blocks[m]
            hidden_width = blocks * (BLOCK // 2) * (6 + ratio_index[m])
            mask = jnp.where(unit < blocks * BLOCK, 1.0, 0.0)
            active = jnp.where(me < depth[m], 1.0, 0.0)
            width = jnp.full((1, BLOCK), blocks * BLOCK, jnp.int32).astype(F32)
            table[m, 0:1, :] = jnp.where(unit < hidden_width, 1.0, 0.0)
            table[m, 1:2, :] = mask
            table[m, 2:3, :] = mask * active
            table[m, 3:4, 0:BLOCK] = 1.0 / width

    def hidden_mask(m, part):
        return table[m // halves, 0:1, part]

    def embed(m, part=features_all):
        return table[m // halves, 1:2, part]

    def live(m, part=features_all):
        return table[m // halves, 2:3, part]

    def width_inv(m):
        return table[m // halves, 3:4, 0:1]

    def stage_device(stage):
        return {"fsdp": 2 * stage + core} if planes else {"section": stage}

    barrier = pltpu.get_barrier_semaphore()
    if planes:
        for step in range(1, section_count):
            signal(barrier, {"section": lax.rem(column + step, section_count)})
            signal(barrier, {"fsdp": lax.rem(shard + 2 * step, shard_count)})
        signal(barrier, {"fsdp": shard + 1 - 2 * core})
        pl.semaphore_wait(barrier, 2 * section_count - 1)
    else:

        @pl.when(jnp.logical_not(is_first))
        def _():
            signal(barrier, {"section": me - 1})

        @pl.when(jnp.logical_not(is_last))
        def _():
            signal(barrier, {"section": me + 1})

        pl.semaphore_wait(barrier, 2 - is_first.astype(jnp.int32) - is_last.astype(jnp.int32))

    def remote(source, target, send, recv, device):
        return pltpu.make_async_remote_copy(
            src_ref=source,
            dst_ref=target,
            send_sem=send,
            recv_sem=recv,
            device_id=device,
            device_id_type=MESH,
        )

    if planes:
        beside = column + 1 - 2 * (column % 2)
        across = column + 2 - 4 * (column // 2)
        corner = 3 - column
        near = (column, beside, across, corner)
        other = {"fsdp": shard + 1 - 2 * core}
        up_rows, down_rows = features // shard_count, hidden_count // shard_count
        up_cols, down_part = hidden_count // section_count, down_rows // section_count
        share = rows // section_count

        def at_rows(start, size):
            return pl.ds(pl.multiple_of(start, size), size)

        def piece(number, full, place, which):
            if number == 0:
                return full.at[at_rows((2 * place + core) * up_rows, up_rows), at_rows(which * up_cols, up_cols)]
            return full.at[at_rows(((2 * place + core) * section_count + which) * down_part, down_part), :]

        def own_piece(number, which):
            if number == 0:
                return own_up.at[:, at_rows(which * up_cols, up_cols)]
            return own_down.at[at_rows(which * down_part, down_part), :]

        fulls = (w_up, w_down)
        holds = (hold_up, hold_down)

        def token_copy(number, m, source):
            raw, land, stage = ((patches, x_in, 0), (cotangent, g_in, stages - 1))[number]
            return remote(
                raw.at[m, at_rows(column * share, share), :],
                land.at[m, at_rows(source * share, share), :],
                token_send.at[number, m],
                token_recv.at[number, m, source],
                stage_device(stage),
            )

        def send_tokens(number, first, last):
            raw, land, stage = ((patches, x_in, 0), (cotangent, g_in, stages - 1))[number]

            @pl.when(chip != stage)
            def _():
                for m in range(first, last):
                    token_copy(number, m, chip).start()

            @pl.when(chip == stage)
            def _():
                for m in range(first, last):
                    land[m, at_rows(chip * share, share), :] = raw[m, at_rows(column * share, share), :]

        def wait_tokens(number, m):
            for source in range(chips):

                @pl.when(chip != source)
                def _():
                    token_copy(number, m, source).wait_recv()

        def scatter_copy(number, far):
            return remote(
                own_piece(number, near[far]),
                holds[number].at[column],
                scatter_send.at[number, far - 1],
                scatter_recv.at[number, column],
                {"section": near[far]},
            )

        def scatter_wait(number, source):
            hold = holds[number]
            remote(
                hold.at[source],
                hold.at[source],
                scatter_send.at[number, 0],
                scatter_recv.at[number, source],
                {"section": beside},
            ).wait_recv()

        def climb_copy(number, source, layer, place):
            return remote(
                source,
                piece(number, fulls[number], place, column),
                climb_send.at[number, layer],
                climb_recv.at[number, place],
                {"fsdp": 2 * layer + core},
            )

        def side_copy(number, way, place, which, kind, device):
            spot = piece(number, fulls[number], place, which)
            return remote(
                spot,
                spot,
                side_send.at[number, way, place],
                side_recv.at[number, kind, place],
                {"section": device},
            )

        def to_beside(number, place):
            return side_copy(number, 0, place, column, 0, beside)

        def to_across(number, place):
            return side_copy(number, 1, place, column, 1, across)

        def relay(number, place):
            if number == 0:
                return side_copy(number, 2, place, beside, 2, across)
            return side_copy(number, 2, place, across, 2, beside)

        def arrived(number, place, kind):
            side_copy(number, 0, place, near[kind + 1], kind, beside).wait_recv()

        def pair_copy(number, place, far, parity):
            which = near[far]
            full = fulls[number]
            if number == 0:
                spot = full.at[at_rows((2 * place + parity) * up_rows, up_rows), at_rows(which * up_cols, up_cols)]
            else:
                first = ((2 * place + parity) * section_count + which) * down_part
                spot = full.at[at_rows(first, down_part), :]
            return remote(
                spot, spot, pair_send.at[number, far, place], pair_recv.at[number, far, place], other
            )

        is_hub = chip == column

        def gain_copy(source, place, way, device):
            return remote(
                source,
                all_gain.at[2 * place + core],
                gain_send.at[way, place],
                gain_recv.at[2 * place + core],
                device,
            )

        def to_hub():
            return gain_copy(own_gain, chip, 0, {"fsdp": 2 * column + core})

        def from_hub(place, far):
            device = other if far == 0 else {"section": near[far]}
            return gain_copy(all_gain.at[2 * place + core], place, far + 1, device)

        def wait_gain(index):
            remote(
                all_gain.at[index], all_gain.at[index], gain_send.at[0, 0], gain_recv.at[index], other
            ).wait_recv()

        def share_gain():
            @pl.when(is_hub)
            def _():
                for place in range(chips):

                    @pl.when(place != chip)
                    def _():
                        wait_gain(2 * place + core)

                    for far in (1, 2, 3, 0):
                        from_hub(place, far).start()

            @pl.when(jnp.logical_not(is_hub))
            def _():
                for place in range(chips):
                    wait_gain(2 * place + core)
                    from_hub(place, 0).start()

        both = (0, 1)
        for number in both:
            for far in (1, 2, 3):
                scatter_copy(number, far).start()
        send_tokens(0, 0, 1)

        @pl.when(is_hub)
        def _():
            all_gain[shard] = own_gain[...]

        @pl.when(jnp.logical_not(is_hub))
        def _():
            to_hub().start()

        build_table()
        for far in (0, 1, 2, 3):
            layer = near[far]
            for number in both:
                if far == 0:
                    source = own_piece(number, column)
                else:
                    scatter_wait(number, layer)
                    source = holds[number].at[layer]

                @pl.when(layer != chip)
                def _():
                    climb_copy(number, source, layer, chip).start()

                @pl.when(layer == chip)
                def _():
                    spot = piece(number, fulls[number], chip, column)
                    spot[...] = source[...]

        def own_turn(step):
            place = lax.rem(chip + step, chips)
            for number in both:
                if step > 0:
                    spot = piece(number, fulls[number], place, column)
                    climb_copy(number, spot, chip, place).wait_recv()
                to_beside(number, place).start()
                to_across(number, place).start()
                pair_copy(number, place, 0, core).start()

        def side_turn(step):
            place = lax.rem(chip + step, chips)
            arrived(0, place, 0)
            relay(0, place).start()
            pair_copy(0, place, 1, core).start()
            arrived(1, place, 1)
            relay(1, place).start()
            pair_copy(1, place, 2, core).start()
            arrived(0, place, 1)
            pair_copy(0, place, 2, core).start()
            arrived(1, place, 0)
            pair_copy(1, place, 1, core).start()

        def corner_turn(step):
            place = lax.rem(chip + step, chips)
            for number in both:
                arrived(number, place, 2)
                pair_copy(number, place, 3, core).start()

        for step in range(chips + 2):
            if step < chips:
                own_turn(step)
            if step == chips - 1:
                send_tokens(0, 1, micro_count)
                send_tokens(1, 0, micro_count)
            if 1 <= step <= chips:
                side_turn(step - 1)
            if 2 <= step:
                corner_turn(step - 2)
            if step == 1:
                share_gain()
        for place in range(chips):
            for far in (0, 1, 2, 3):
                for number in both:
                    pair_copy(number, place, far, 1 - core).wait_recv()
        for place in range(chips):
            wait_gain(2 * place + 1 - core)
        gain_blocks = jnp.sum(all_gain[...], axis=0)
        gain = jnp.concatenate(
            [gain_blocks[i : i + 1, :] for i in range(features // BLOCK)], axis=1
        )
    else:
        build_table()
        w_up, w_down, acc_gain = own_up, own_down, grad_gain
        gain = own_gain[:1]

    columns = chunks(features, 256)

    def forward_copy(m, index):
        start, size = columns[index]
        return pltpu.make_async_remote_copy(
            src_ref=x_out.at[m, :, pl.ds(start, size)],
            dst_ref=x_in.at[m, :, pl.ds(start, size)],
            send_sem=fwd_send.at[m, index],
            recv_sem=fwd_recv.at[m, index],
            device_id=stage_device(jnp.minimum(me + 1, stages - 1)),
            device_id_type=MESH,
        )

    def backward_copy(m):
        return pltpu.make_async_remote_copy(
            src_ref=g_out.at[m],
            dst_ref=g_in.at[m],
            send_sem=bwd_send.at[m],
            recv_sem=bwd_recv.at[m],
            device_id=stage_device(jnp.maximum(me - 1, 0)),
            device_id_type=MESH,
        )

    def layer_norm(m):
        mask = embed(m)
        scale = width_inv(m)
        values = x_in[m].astype(F32) * mask
        center = jnp.sum(values, axis=-1, keepdims=True) * scale
        centered = (values - center) * mask
        variance = jnp.sum(centered * centered, axis=-1, keepdims=True) * scale
        inv_std = lax.rsqrt(variance + EPSILON)
        return centered * inv_std, inv_std

    def forward(m):
        at = pl.ds(pl.multiple_of(m * rows, rows), rows)

        @pl.when(is_first)
        def _():
            if planes:
                wait_tokens(0, m)
                x_in[m] = (x_in[m].astype(F32) * embed(m)).astype(BF16)
            else:
                x_in[m] = (patches[m].astype(F32) * embed(m)).astype(BF16)

        @pl.when(jnp.logical_not(is_first))
        def _():
            for index in range(len(columns)):
                forward_copy(m, index).wait_recv()

        standard, _ = layer_norm(m)
        scaled = standard * gain
        normed = scaled.astype(BF16)
        for start, size in chunks(hidden_count, 512):
            part = pl.ds(start, size)
            hidden = jnp.dot(normed, w_up[:, part], preferred_element_type=F32)
            value, rise = gelu_and_slope(hidden)
            mask = hidden_mask(m, part)
            act[at, part] = (value * mask).astype(BF16)
            slope[at, part] = (rise * mask).astype(BF16)

        @pl.when(jnp.logical_not(is_last))
        def _():
            for index, (start, size) in enumerate(columns):
                part = pl.ds(start, size)
                branch = jnp.dot(act[at, :], w_down[:, part], preferred_element_type=F32)
                out = x_in[m, :, part].astype(F32) + live(m, part) * branch
                x_out[m, :, part] = out.astype(BF16)
                forward_copy(m, index).start()

        return scaled

    def whole_micro(number):
        return pl.ds(pl.multiple_of(number * halves * rows, halves * rows), halves * rows)

    def forward_micro(number, carry):
        parts = [forward(number * halves + half) for half in range(halves)]
        normed_t[:, whole_micro(number)] = jnp.transpose(jnp.concatenate(parts, axis=0)).astype(BF16)
        return carry

    acc_gain[...] = jnp.zeros_like(acc_gain)

    def backward(m):
        at = pl.ds(pl.multiple_of(m * rows, rows), rows)

        @pl.when(is_last)
        def _():
            if planes:
                wait_tokens(1, m)
                g_in[m] = (g_in[m].astype(F32) * embed(m)).astype(BF16)
            else:
                g_in[m] = (cotangent[m].astype(F32) * embed(m)).astype(BF16)

        @pl.when(jnp.logical_not(is_last))
        def _():
            backward_copy(m).wait_recv()

        grad_float = g_in[m].astype(F32)
        branch_float = grad_float * live(m)
        branch = branch_float.astype(BF16)
        for start, size in chunks(hidden_count, 512):
            part = pl.ds(start, size)
            grad_act = contract_last(branch, w_down[part, :])
            slope[at, part] = (grad_act * slope[at, part].astype(F32)).astype(BF16)
        grad_hidden = slope[at, :]
        grad_normed = jnp.concatenate(
            [
                contract_last(grad_hidden, w_up[pl.ds(start, size), :])
                for start, size in chunks(features, 256)
            ],
            axis=1,
        )
        standard, inv_std = layer_norm(m)
        mask = embed(m)
        scale = width_inv(m)
        acc_gain[...] += jnp.sum((grad_normed * standard).reshape(-1, 8, features), axis=0)

        @pl.when(jnp.logical_not(is_first))
        def _():
            grad_standard = grad_normed * gain * mask
            first = jnp.sum(grad_standard, axis=-1, keepdims=True) * scale
            second = jnp.sum(grad_standard * standard, axis=-1, keepdims=True) * scale
            grad_x = inv_std * (grad_standard - first * mask - standard * second)
            g_out[m] = (grad_float + grad_x).astype(BF16)
            backward_copy(m).start()

        return branch_float

    def backward_micro(number, carry):
        parts = [backward(number * halves + half) for half in range(halves)]
        branch_t[:, whole_micro(number)] = jnp.transpose(jnp.concatenate(parts, axis=0)).astype(BF16)
        return carry

    micro_total = micro_count // halves
    lag = jnp.minimum(LAG * (stages - 1 - me), micro_total)

    def turn(number, carry):
        @pl.when(number < micro_total)
        def _():
            forward_micro(jnp.minimum(number, micro_total - 1), 0)

        late = number - lag

        @pl.when(jnp.logical_and(late >= 0, late < micro_total))
        def _():
            backward_micro(jnp.clip(late, 0, micro_total - 1), 0)

        return carry

    lax.fori_loop(0, 2 * micro_total, turn, 0)

    width = 256 if hidden_count % 256 == 0 else hidden_count

    def up_grads(first, size, step):
        part = pl.ds(pl.multiple_of(step * width, width), width)
        these = pl.ds(first, size)
        return these, part, jnp.dot(normed_t[these, :], slope[:, part], preferred_element_type=F32)

    def down_grads(part):
        down = jnp.dot(branch_t[...], act[:, part], preferred_element_type=F32)
        return jnp.transpose(down).astype(BF16)

    def weight_grads(step, carry):
        these, part, up = up_grads(0, features, step)
        grad_up[these, part] = up.astype(BF16)
        grad_down[part, :] = down_grads(part)
        return carry

    def slot(full, index):
        size = full.shape[0] // shard_count
        return full.at[pl.ds(pl.multiple_of(index * size, size), size)]

    if planes:
        pairs = (pair_up, pair_down)
        firsts = (first_up, first_down)
        seconds = (second_up, second_down)
        finals = (plane_up, plane_down)
        lasts = (last_up, last_down)
        first_way = (beside, across)
        second_way = (across, beside)
        kept = (across, beside)

        def sum_pair(number, place):
            return remote(
                slot(fulls[number], 2 * place + 1 - core),
                pairs[number].at[place],
                sum_pair_send.at[number, place],
                sum_pair_recv.at[number, place],
                other,
            )

        def first_copy(number, place, index):
            which = (first_way[number], corner)[index]
            return remote(
                piece(number, fulls[number], place, which),
                firsts[number].at[place, index],
                first_send.at[number, place, index],
                first_recv.at[number, place, index],
                {"section": first_way[number]},
            )

        def second_copy(number, place):
            return remote(
                piece(number, fulls[number], place, kept[number]),
                seconds[number].at[place],
                second_send.at[number, place],
                second_recv.at[number, place],
                {"section": second_way[number]},
            )

        def plane_copy(number, place, layer):
            return remote(
                piece(number, fulls[number], place, column),
                finals[number].at[layer],
                plane_send.at[number, place],
                plane_recv.at[number, layer],
                {"fsdp": 2 * place + core},
            )

        def last_copy(number, layer, source):
            return remote(
                finals[number].at[layer],
                lasts[number].at[source],
                last_send.at[number, layer],
                last_recv.at[number, source],
                {"section": layer},
            )

        def make_grads(place):
            up_size = 2 * up_rows
            first_row = pl.multiple_of(place * up_size, up_size)

            def up_step(step, carry):
                these, part, up = up_grads(first_row, up_size, step)
                w_up[these, part] = up.astype(BF16)
                return carry

            lax.fori_loop(0, hidden_count // width, up_step, 0)
            sum_pair(0, place).start()
            down_size = 2 * down_rows
            size = math.gcd(down_size, width)

            def down_step(step, carry):
                part = at_rows(place * down_size + step * size, size)
                w_down[part, :] = down_grads(part)
                return carry

            lax.fori_loop(0, down_size // size, down_step, 0)
            sum_pair(1, place).start()

        def first_turn(place):
            for number in both:
                mine = slot(fulls[number], 2 * place + core)
                sum_pair(number, place).wait_recv()
                mine[...] = (mine[...].astype(F32) + pairs[number][place].astype(F32)).astype(BF16)
                for index in (0, 1):
                    first_copy(number, place, index).start()

        def second_turn(place):
            for number in both:
                for index in (1, 0):
                    first_copy(number, place, index).wait_recv()
                spot = piece(number, fulls[number], place, kept[number])
                total = spot[...].astype(F32) + firsts[number][place, 1].astype(F32)
                spot[...] = total.astype(BF16)
                second_copy(number, place).start()

        def plane_turn(place):
            for number in both:
                second_copy(number, place).wait_recv()
                spot = piece(number, fulls[number], place, column)
                total = spot[...].astype(F32) + firsts[number][place, 0].astype(F32)
                total = (total + seconds[number][place].astype(F32)).astype(BF16)

                @pl.when(place != chip)
                def _():
                    spot[...] = total
                    plane_copy(number, place, chip).start()

                @pl.when(place == chip)
                def _():
                    finals[number][chip] = total

        def place_at(index):
            return lax.rem(chip + chips - 1 - index + chips, chips)

        def reduce_step(index, carry):
            @pl.when(index < chips)
            def _():
                make_grads(place_at(index))
                first_turn(place_at(index))

            @pl.when(jnp.logical_and(index >= 1, index <= chips))
            def _():
                second_turn(place_at(jnp.maximum(index - 1, 0)))

            @pl.when(jnp.logical_and(index == chips, is_hub))
            def _():
                hub_turn()

            @pl.when(index >= 2)
            def _():
                plane_turn(place_at(jnp.maximum(index - 2, 0)))

            return carry

        rise = jnp.sum(acc_gain[...], axis=0, keepdims=True)
        spare = own_gain.shape[0] - features // BLOCK
        rise_rows = [rise[:, i : i + BLOCK] for i in range(0, features, BLOCK)]
        if spare:
            rise_rows.append(jnp.zeros((spare, BLOCK), F32))
        rise_own[...] = jnp.concatenate(rise_rows, axis=0)

        def rise_copy(source, target, way, device):
            return remote(source, all_rise.at[target], rise_send.at[way], rise_recv.at[target], device)

        def rise_to_hub():
            return rise_copy(rise_own, column, 0, {"section": chip})

        def rise_to_pair():
            return rise_copy(rise_own, chips, 1, other)

        def rise_to_place(place):
            return rise_copy(rise_sum, chips + 1, 2 + place, {"fsdp": 2 * place + core})

        def rise_wait(target):
            rise_copy(all_rise.at[target], target, 0, other).wait_recv()

        @pl.when(jnp.logical_not(is_hub))
        def _():
            rise_to_hub().start()

        def hub_turn():
            total = rise_own[...]
            for far in (1, 2, 3):
                rise_wait(near[far])
                total = total + all_rise[near[far]]
            rise_own[...] = total
            rise_to_pair().start()
            rise_wait(chips)
            rise_sum[...] = total + all_rise[chips]
            for place in range(chips):

                @pl.when(place != chip)
                def _():
                    rise_to_place(place).start()

        for number in both:
            for far in (1, 2, 3):
                scatter_copy(number, far).wait_send()
            for layer in range(chips):

                @pl.when(chip != layer)
                def _():
                    climb_copy(number, holds[number].at[layer], layer, chip).wait_send()

            for place in range(chips):
                to_beside(number, place).wait_send()
                to_across(number, place).wait_send()
                relay(number, place).wait_send()
                for far in (0, 1, 2, 3):
                    pair_copy(number, place, far, core).wait_send()

        @pl.when(is_hub)
        def _():
            for place in range(chips):
                for far in (0, 1, 2, 3):
                    from_hub(place, far).wait_send()

        @pl.when(jnp.logical_not(is_hub))
        def _():
            to_hub().wait_send()
            for place in range(chips):
                from_hub(place, 0).wait_send()

        lax.fori_loop(0, chips + 2, reduce_step, 0)
        for layer in reversed(range(chips)):
            for number in both:

                @pl.when(layer != chip)
                def _():
                    plane_copy(number, chip, layer).wait_recv()

                @pl.when(layer != column)
                def _():
                    last_copy(number, layer, column).start()

                @pl.when(layer == column)
                def _():
                    lasts[number][layer] = finals[number][layer]

        @pl.when(is_hub)
        def _():
            grad_gain[...] = rise_sum[...]
            rise_to_pair().wait_send()
            for place in range(chips):

                @pl.when(place != chip)
                def _():
                    rise_to_place(place).wait_send()

        @pl.when(jnp.logical_not(is_hub))
        def _():
            rise_wait(chips + 1)
            grad_gain[...] = all_rise[chips + 1]
            rise_to_hub().wait_send()

        for source in range(section_count):
            for number in both:

                @pl.when(source != column)
                def _():
                    last_copy(number, source, source).wait_recv()

            grad_up[:, pl.ds(source * up_cols, up_cols)] = last_up[source]
            grad_down[pl.ds(source * down_part, down_part), :] = last_down[source]
        for number in both:
            for place in range(chips):
                sum_pair(number, place).wait_send()
                second_copy(number, place).wait_send()
                for index in (0, 1):
                    first_copy(number, place, index).wait_send()

                @pl.when(place != chip)
                def _():
                    plane_copy(number, place, chip).wait_send()

                @pl.when(place != column)
                def _():
                    last_copy(number, place, column).wait_send()

        for number, stage in ((0, 0), (1, stages - 1)):

            @pl.when(chip != stage)
            def _():
                for m in range(micro_count):
                    token_copy(number, m, chip).wait_send()
    else:
        lax.fori_loop(0, hidden_count // width, weight_grads, 0)

    def drain(m, carry):
        @pl.when(jnp.logical_not(is_last))
        def _():
            for index in range(len(columns)):
                forward_copy(m, index).wait_send()

        @pl.when(jnp.logical_not(is_first))
        def _():
            backward_copy(m).wait_send()

        return carry

    lax.fori_loop(0, micro_count, drain, 0)


def run_pipeline(planes, patches, cotangent, scalars, gain, w_up, w_down):
    section_count = lax.axis_size("section")
    shard_count = lax.axis_size("fsdp")
    micro_count, rows, features = patches.shape
    hidden_count = w_up.shape[1]
    vmem = pl.BlockSpec(memory_space=pltpu.VMEM)
    token = (micro_count, rows, features)
    tokens = micro_count * rows
    chips = shard_count // 2
    dma = pltpu.SemaphoreType.DMA
    scratch = [
        pltpu.VMEM(token, BF16),
        pltpu.VMEM(token, BF16),
        pltpu.VMEM(token, BF16),
        pltpu.VMEM(token, BF16),
        pltpu.VMEM((tokens, hidden_count), BF16),
        pltpu.VMEM((tokens, hidden_count), BF16),
        pltpu.VMEM((features, tokens), BF16),
        pltpu.VMEM((features, tokens), BF16),
        pltpu.VMEM(scalars[0].shape + (8, hidden_count), F32),
        dma((micro_count, len(chunks(features, 256)))),
        dma((micro_count, len(chunks(features, 256)))),
        dma((micro_count,)),
        dma((micro_count,)),
    ]
    if planes:
        up_rows, down_rows = features // shard_count, hidden_count // shard_count
        up_piece = (up_rows, hidden_count // section_count)
        down_piece = (down_rows // section_count, features)
        scratch += [
            pltpu.VMEM((features, hidden_count), BF16),
            pltpu.VMEM((hidden_count, features), BF16),
            pltpu.VMEM((section_count,) + up_piece, BF16),
            pltpu.VMEM((section_count,) + down_piece, BF16),
            pltpu.VMEM((shard_count,) + gain.shape, F32),
            pltpu.VMEM((chips + 2,) + gain.shape, F32),
            pltpu.VMEM(gain.shape, F32),
            pltpu.VMEM(gain.shape, F32),
            pltpu.VMEM((8, features), F32),
            pltpu.VMEM((chips, up_rows, hidden_count), BF16),
            pltpu.VMEM((chips, down_rows, features), BF16),
            pltpu.VMEM((chips, 2) + up_piece, BF16),
            pltpu.VMEM((chips, 2) + down_piece, BF16),
            pltpu.VMEM((chips,) + up_piece, BF16),
            pltpu.VMEM((chips,) + down_piece, BF16),
            pltpu.VMEM((chips,) + up_piece, BF16),
            pltpu.VMEM((chips,) + down_piece, BF16),
            pltpu.VMEM((section_count,) + up_piece, BF16),
            pltpu.VMEM((section_count,) + down_piece, BF16),
            dma((2, micro_count)),
            dma((2, micro_count, chips)),
            dma((5, chips)),
            dma((shard_count,)),
            dma((2 + chips,)),
            dma((2 + chips,)),
            dma((2, 3)),
            dma((2, section_count)),
            dma((2, chips)),
            dma((2, chips)),
            dma((2, 3, chips)),
            dma((2, 3, chips)),
            dma((2, 4, chips)),
            dma((2, 4, chips)),
            dma((2, chips)),
            dma((2, chips)),
            dma((2, chips, 2)),
            dma((2, chips, 2)),
            dma((2, chips)),
            dma((2, chips)),
            dma((2, chips)),
            dma((2, chips)),
            dma((2, chips)),
            dma((2, section_count)),
        ]
        grads = (
            jax.ShapeDtypeStruct((up_rows, hidden_count), BF16),
            jax.ShapeDtypeStruct((down_rows, features), BF16),
        )
    else:
        grads = (
            jax.ShapeDtypeStruct((features, hidden_count), BF16),
            jax.ShapeDtypeStruct((hidden_count, features), BF16),
        )
    return pl.pallas_call(
        functools.partial(pipeline_kernel, section_count, shard_count),
        out_shape=grads + (jax.ShapeDtypeStruct(gain.shape, F32),),
        in_specs=[vmem] * 2 + [pl.BlockSpec(memory_space=pltpu.SMEM)] * 3 + [vmem] * 3,
        out_specs=(vmem, vmem, vmem),
        scratch_shapes=scratch,
        compiler_params=pltpu.CompilerParams(
            collective_id=0, has_side_effects=True, vmem_limit_bytes=VMEM_BYTES
        ),
    )(patches, cotangent, *scalars, gain, w_up, w_down)


def per_device(patches, cotangent, embed_blocks, ratio_index, depth, w_up, w_down, ln_gain):
    shard_index = lax.axis_index("fsdp")
    shard_count = lax.axis_size("fsdp")
    micro_count, rows, features = patches.shape
    hidden_count = w_up.shape[2]
    gain_count = ln_gain.shape[1]
    section_count = lax.axis_size("section")
    down_part = w_down.shape[1] // section_count
    planes = (
        section_count == 4
        and shard_count == 2 * section_count
        and gain_count % 16 == 0
        and down_part % 16 == 0
        and hidden_count % (128 * section_count) == 0
        and rows % (16 * section_count) == 0
    )

    scalars = (embed_blocks, ratio_index, depth)
    start = shard_index * gain_count

    if planes:
        halves = 2 if rows % (32 * section_count) == 0 and SPLIT else 1
        gain_rows = -(-features // (8 * BLOCK)) * 8
        spot = lax.iota(jnp.int32, gain_rows * BLOCK)
        repeats = -(-gain_rows * BLOCK // gain_count)
        gain = jnp.tile(ln_gain[0].astype(F32), repeats)[: gain_rows * BLOCK]
        gain = jnp.where(spot // gain_count == shard_index, gain, 0.0).reshape(gain_rows, BLOCK)
        split = (micro_count * halves, rows // halves, features)
        own_up, own_down, gains = run_pipeline(
            True, patches.reshape(split), cotangent.reshape(split), scalars, gain, w_up[0], w_down[0]
        )
        own_gain = lax.dynamic_slice(gains.reshape(-1), (start,), (gain_count,))
        return (own_up.astype(F32)[None], own_down.astype(F32)[None], own_gain[None])

    full_up = lax.all_gather(w_up[0], "fsdp", axis=0, tiled=True)
    full_down = lax.all_gather(w_down[0], "fsdp", axis=0, tiled=True)
    gain = lax.all_gather(ln_gain[0], "fsdp", axis=0, tiled=True).astype(F32)
    gain = jnp.broadcast_to(gain[None], (8, features))
    part_up, part_down, gains = run_pipeline(
        False, patches, cotangent, scalars, gain, full_up, full_down
    )
    own_down = lax.psum_scatter(part_down, "fsdp", scatter_dimension=0, tiled=True)
    own_up = lax.psum_scatter(part_up, "fsdp", scatter_dimension=0, tiled=True)
    part_gain = jnp.sum(gains, axis=0)
    own_gain = lax.psum_scatter(part_gain, "fsdp", scatter_dimension=0, tiled=True)
    return (own_up.astype(F32)[None], own_down.astype(F32)[None], own_gain[None])


def solution(mesh):
    return jax.shard_map(
        per_device,
        mesh=mesh,
        in_specs=(
            P(None, "fsdp", None),
            P(None, "fsdp", None),
            P(),
            P(),
            P(),
            P("section", "fsdp", None),
            P("section", "fsdp", None),
            P("section", "fsdp"),
        ),
        out_specs=(P("section", "fsdp", None), P("section", "fsdp", None), P("section", "fsdp")),
        check_vma=False,
    )
```
